32 devices in a mesh: dp: 4 (over y, z), tp: 8 (over x, core).
Axes of the slice: x: 4, y: 2, z: 2, core: 2. Of those that a mesh axis runs over, the one named last changes fastest.
The devices are a block of a 4x4x8 slice.
Arguments:
- hidden: bfloat16 [64, 64, 2048], P('dp'), parts along dimension 0
- tree_mask: int32 [64, 64, 64], P('dp'), parts along dimension 0
- depth: int32 [64, 64], P('dp'), parts along dimension 0
- ctx_len: int32 [64], P('dp'), parts along dimension 0
- block_table: int32 [64, 24], P('dp'), parts along dimension 0
- score_id: int32 [64, 64], P('dp'), parts along dimension 0
- k_cache: bfloat16 [1536, 16, 8, 64], P('dp', None, 'tp'), parts along dimension 0
- v_cache: bfloat16 [1536, 16, 8, 64], P('dp', None, 'tp'), parts along dimension 0
- attn_norm: bfloat16 [2048], replicated
- w_q: bfloat16 [2048, 2048], P(None, 'tp')
- w_k: bfloat16 [2048, 512], P(None, 'tp')
- w_v: bfloat16 [2048, 512], P(None, 'tp')
- w_o: bfloat16 [2048, 2048], P('tp')
- mlp_norm: bfloat16 [2048], replicated
- w_gate: bfloat16 [2048, 8192], P(None, 'tp')
- w_up: bfloat16 [2048, 8192], P(None, 'tp')
- w_down: bfloat16 [8192, 2048], P('tp')
- final_norm: bfloat16 [2048], replicated
- w_lm: bfloat16 [2048, 128256], P(None, 'tp')
Outputs:
- output 1: float32 [64, 64], P('dp'), parts along dimension 0
- output 2: float32 [64, 64], P('dp'), parts along dimension 0
- output 3: bfloat16 [1536, 16, 8, 64], P('dp', None, 'tp'), parts along dimension 0
- output 4: bfloat16 [1536, 16, 8, 64], P('dp', None, 'tp'), parts along dimension 0
There are 4 independent parts. The reference program is written for one: setup_inputs(seed, part) draws one part's arguments, and reference() takes and returns one part's arrays. A program takes and returns all parts, laid end to end along the dimension named above; an argument that names none is the same for every part.
All inputs are finite; a program needn't handle non-finite values.
Results may differ from the reference program's by a relative error of at most 0.00344325.
Values are sent between devices in bfloat16 or wider.
A program may use at most 768 MiB of HBM per device.

```python
import math
import jax
import jax.numpy as jnp
from jax import lax

REQUESTS = 16
NODES = 64
PAGES = 24
PAGE_SIZE = 16
MODEL_DIM = 2048
HEADS = 32
KV_HEADS = 8
HEAD_DIM = 64
FFN_DIM = 8192
VOCAB_SIZE = 128256
ROPE_THETA = 500000
RMS_EPS = 1e-5
BLOCKS = REQUESTS * PAGES
SPAN = PAGES * PAGE_SIZE
MAX_CTX = SPAN - NODES
GROUP = HEADS // KV_HEADS


def draw_routing(key):
    k_spread, k_step, k_ctx, k_table, k_score = jax.random.split(key, 5)
    spread = jax.random.randint(k_spread, (REQUESTS, 1), 1, 4)
    step = jnp.minimum(jax.random.randint(k_step, (REQUESTS, NODES), 0, 4), spread)
    node_ids = jnp.arange(NODES)
    parent = jnp.maximum(node_ids[None, :] - 1 - step, 0)
    linked = (parent[:, :, None] == node_ids[None, None, :]) & (node_ids[None, :, None] > 0)
    reach = linked | (node_ids[:, None] == node_ids[None, :])[None]
    for _ in range(int(math.log2(NODES)) + 1):
        reach = jnp.any(reach[:, :, :, None] & reach[:, None, :, :], axis=2)
    tree_mask = reach.astype(jnp.int32)
    depth = jnp.sum(tree_mask, axis=-1).astype(jnp.int32) - 1
    ctx_len = jax.random.randint(k_ctx, (REQUESTS,), 1, MAX_CTX + 1).astype(jnp.int32)
    ctx_len = ctx_len.at[0].set(MAX_CTX)
    block_table = jax.random.permutation(k_table, BLOCKS).astype(jnp.int32).reshape(REQUESTS, PAGES)
    score_id = jax.random.randint(k_score, (REQUESTS, NODES), 0, VOCAB_SIZE).astype(jnp.int32)
    score_id = score_id.at[0, 0].set(VOCAB_SIZE - 1)
    return tree_mask, depth, ctx_len, block_table, score_id


def normal_weight(key, shape, scale):
    return (scale * jax.random.normal(key, shape, jnp.float32)).astype(jnp.bfloat16)


def gain_vector(key):
    return (1.0 + 0.3 * jax.random.normal(key, (MODEL_DIM,), jnp.float32)).astype(jnp.bfloat16)


def setup_inputs(seed: int = 0, part: int = 0) -> dict:
    part_key = jax.random.fold_in(jax.random.key(seed), part)
    keys = jax.random.split(part_key, 4)
    tree_mask, depth, ctx_len, block_table, score_id = draw_routing(keys[0])
    shared = jax.random.split(jax.random.key(seed + 1), 11)
    cache_shape = (BLOCKS, PAGE_SIZE, KV_HEADS, HEAD_DIM)
    return {
        "hidden": normal_weight(keys[1], (REQUESTS, NODES, MODEL_DIM), 1.0),
        "tree_mask": tree_mask,
        "depth": depth,
        "ctx_len": ctx_len,
        "block_table": block_table,
        "score_id": score_id,
        "k_cache": normal_weight(keys[2], cache_shape, 1.0),
        "v_cache": normal_weight(keys[3], cache_shape, 1.0),
        "attn_norm": gain_vector(shared[0]),
        "w_q": normal_weight(shared[1], (MODEL_DIM, HEADS * HEAD_DIM), 2.5 * MODEL_DIM ** -0.5),
        "w_k": normal_weight(shared[2], (MODEL_DIM, KV_HEADS * HEAD_DIM), 1.5 * MODEL_DIM ** -0.5),
        "w_v": normal_weight(shared[3], (MODEL_DIM, KV_HEADS * HEAD_DIM), MODEL_DIM ** -0.5),
        "w_o": normal_weight(shared[4], (HEADS * HEAD_DIM, MODEL_DIM), 1.5 * (HEADS * HEAD_DIM) ** -0.5),
        "mlp_norm": gain_vector(shared[5]),
        "w_gate": normal_weight(shared[6], (MODEL_DIM, FFN_DIM), MODEL_DIM ** -0.5),
        "w_up": normal_weight(shared[7], (MODEL_DIM, FFN_DIM), MODEL_DIM ** -0.5),
        "w_down": normal_weight(shared[8], (FFN_DIM, MODEL_DIM), 1.5 * FFN_DIM ** -0.5),
        "final_norm": gain_vector(shared[9]),
        "w_lm": normal_weight(shared[10], (MODEL_DIM, VOCAB_SIZE), 3.0 * MODEL_DIM ** -0.5),
    }


def rms_norm(values, gain):
    widened = values.astype(jnp.float32)
    scale = lax.rsqrt(jnp.mean(widened * widened, axis=-1, keepdims=True) + RMS_EPS)
    return (widened * scale * gain.astype(jnp.float32)).astype(jnp.bfloat16)


def rotate(values, positions):
    head_dim = values.shape[-1]
    half = head_dim // 2
    inv_freq = 1.0 / (ROPE_THETA ** (jnp.arange(half, dtype=jnp.float32) * (2.0 / head_dim)))
    angles = positions.astype(jnp.float32)[..., None] * inv_freq
    cosine = jnp.cos(angles)[..., None, :]
    sine = jnp.sin(angles)[..., None, :]
    first = values[..., :half]
    second = values[..., half:]
    return jnp.concatenate([first * cosine - second * sine, second * cosine + first * sine], axis=-1)


def reference(hidden, tree_mask, depth, ctx_len, block_table, score_id, k_cache, v_cache, attn_norm, w_q, w_k, w_v, w_o, mlp_norm, w_gate, w_up, w_down, final_norm, w_lm):
    scale = HEAD_DIM ** -0.5
    slot_ids = jnp.arange(SPAN)

    def one_request(item):
        rows, mask_row, depth_row, context, table_row, targets = item
        normed = rms_norm(rows, attn_norm)
        positions = context + depth_row
        query = jnp.dot(normed, w_q, preferred_element_type=jnp.float32).reshape(NODES, HEADS, HEAD_DIM)
        query = rotate(query, positions).astype(jnp.bfloat16).reshape(NODES, KV_HEADS, GROUP, HEAD_DIM)
        key_new = jnp.dot(normed, w_k, preferred_element_type=jnp.float32).reshape(NODES, KV_HEADS, HEAD_DIM)
        key_new = rotate(key_new, positions).astype(jnp.bfloat16)
        val_new = jnp.dot(normed, w_v, preferred_element_type=jnp.float32).astype(jnp.bfloat16).reshape(NODES, KV_HEADS, HEAD_DIM)
        key_old = k_cache[table_row].reshape(SPAN, KV_HEADS, HEAD_DIM)
        val_old = v_cache[table_row].reshape(SPAN, KV_HEADS, HEAD_DIM)
        query_wide = query.astype(jnp.float32)
        score_old = jnp.einsum("tkgh,skh->tkgs", query_wide, key_old.astype(jnp.float32)) * scale
        score_old = jnp.where((slot_ids < context)[None, None, None, :], score_old, -jnp.inf)
        score_new = jnp.einsum("tkgh,jkh->tkgj", query_wide, key_new.astype(jnp.float32)) * scale
        score_new = jnp.where((mask_row > 0)[:, None, None, :], score_new, -jnp.inf)
        top = jnp.maximum(jnp.max(score_old, axis=-1), jnp.max(score_new, axis=-1))[..., None]
        prob_old = jnp.exp(score_old - top)
        prob_new = jnp.exp(score_new - top)
        total = jnp.sum(prob_old, axis=-1) + jnp.sum(prob_new, axis=-1)
        mixed = jnp.einsum("tkgs,skh->tkgh", prob_old.astype(jnp.bfloat16).astype(jnp.float32), val_old.astype(jnp.float32))
        mixed = mixed + jnp.einsum("tkgj,jkh->tkgh", prob_new.astype(jnp.bfloat16).astype(jnp.float32), val_new.astype(jnp.float32))
        attended = (mixed / total[..., None]).astype(jnp.bfloat16).reshape(NODES, HEADS * HEAD_DIM)
        attn_out = jnp.dot(attended, w_o, preferred_element_type=jnp.float32).astype(jnp.bfloat16)
        residual = (rows.astype(jnp.float32) + attn_out.astype(jnp.float32)).astype(jnp.bfloat16)
        normed_mlp = rms_norm(residual, mlp_norm)
        gate = jnp.dot(normed_mlp, w_gate, preferred_element_type=jnp.float32)
        upper = jnp.dot(normed_mlp, w_up, preferred_element_type=jnp.float32)
        product = (jax.nn.silu(gate) * upper).astype(jnp.bfloat16)
        mlp_out = jnp.dot(product, w_down, preferred_element_type=jnp.float32).astype(jnp.bfloat16)
        layer_out = (residual.astype(jnp.float32) + mlp_out.astype(jnp.float32)).astype(jnp.bfloat16)
        logits = jnp.dot(rms_norm(layer_out, final_norm), w_lm, preferred_element_type=jnp.float32)
        log_norm = jax.nn.logsumexp(logits, axis=-1)
        picked = jnp.take_along_axis(logits, targets[:, None], axis=-1)[:, 0]
        return log_norm, picked - log_norm, key_new, val_new

    log_norm, log_prob, key_new, val_new = lax.map(one_request, (hidden, tree_mask, depth, ctx_len, block_table, score_id))
    slots = ctx_len[:, None] + jnp.arange(NODES)[None, :]
    slot_blocks = jnp.take_along_axis(block_table, slots // PAGE_SIZE, axis=1)
    k_out = k_cache.at[slot_blocks, slots % PAGE_SIZE].set(key_new)
    v_out = v_cache.at[slot_blocks, slots % PAGE_SIZE].set(val_new)
    return (log_norm, log_prob, k_out, v_out)
```

```python
import functools

import jax
import jax.numpy as jnp
from jax import lax
from jax.experimental import pallas as pl
from jax.experimental.pallas import tpu as pltpu
from jax.sharding import PartitionSpec as P

RMS_EPS = 1e-5
ROPE_THETA = 500000
CHIPS = 4
CHUNKS = 2
TILE = 512
COLS = 512
STEP = 32
VMEM_LIMIT = 67043328
F32 = jnp.float32
BF16 = jnp.bfloat16


def rms_norm(values, gain):
    widened = values.astype(F32)
    scale = lax.rsqrt(jnp.mean(widened * widened, axis=-1, keepdims=True) + RMS_EPS)
    return (widened * scale * gain.astype(F32)).astype(BF16)


def rotate(values, positions):
    head_dim = values.shape[-1]
    half = head_dim // 2
    inv_freq = 1.0 / (ROPE_THETA ** (jnp.arange(half, dtype=F32) * (2.0 / head_dim)))
    angles = positions.astype(F32)[..., None] * inv_freq
    cosine = jnp.cos(angles)[..., None, :]
    sine = jnp.sin(angles)[..., None, :]
    first = values[..., :half]
    second = values[..., half:]
    return jnp.concatenate([first * cosine - second * sine, second * cosine + first * sine], axis=-1)


def tree_attention(query, key_new, val_new, key_old, val_old, tree_mask, ctx_len):
    scale = query.shape[-1] ** -0.5
    span = key_old.shape[1]
    score_old = jnp.einsum("btkgh,bskh->btkgs", query, key_old, preferred_element_type=F32) * scale
    seen_old = jnp.arange(span)[None, :] < ctx_len[:, None]
    score_old = jnp.where(seen_old[:, None, None, None, :], score_old, -jnp.inf)
    score_new = jnp.einsum("btkgh,bjkh->btkgj", query, key_new, preferred_element_type=F32) * scale
    score_new = jnp.where((tree_mask > 0)[:, :, None, None, :], score_new, -jnp.inf)
    top = jnp.maximum(jnp.max(score_old, axis=-1), jnp.max(score_new, axis=-1))[..., None]
    prob_old = jnp.exp(score_old - top)
    prob_new = jnp.exp(score_new - top)
    total = jnp.sum(prob_old, axis=-1) + jnp.sum(prob_new, axis=-1)
    mixed = jnp.einsum("btkgs,bskh->btkgh", prob_old.astype(BF16), val_old, preferred_element_type=F32)
    mixed = mixed + jnp.einsum("btkgj,bjkh->btkgh", prob_new.astype(BF16), val_new, preferred_element_type=F32)
    return (mixed / total[..., None]).astype(BF16)


def write_cache(cache, table, ctx_len, new_rows):
    page_size = cache.shape[1]
    slots = ctx_len[:, None] + jnp.arange(new_rows.shape[1])[None, :]
    slot_blocks = jnp.take_along_axis(table, slots // page_size, axis=1)
    return cache.at[slot_blocks, slots % page_size].set(new_rows)


class Copies:
    def __init__(self, make, plan):
        self.make = make
        self.plan = plan

    def __getitem__(self, k):
        return self.make(*self.plan[k]())

    def all(self):
        return [self[k] for k in range(len(self.plan))]


def tail_body(tp, att_hbm, hid_hbm, wo_hbm, wg_hbm, wu_hbm, wd_hbm, lm_hbm, gain_m, gain_f, target, norm_out, prob_out,
              att_own, att_far, hid, wo, wg, wu, wd, part, mrg_in, mrg_out, fin_in, h1, gat, fin, act, tiles, lga, lgb, run, stats,
              s_load, s_pair_s, s_pair_r, s_rs_s, s_rs_r, s_ag_s, s_ag_r, s_dd_s, s_dd_r, s_tile, s_st_s, s_st_r):
    me = lax.axis_index("tp")
    x = me // 2
    core = me % 2
    right = 2 * ((x + 1) % CHIPS) + core
    left = 2 * ((x + CHIPS - 1) % CHIPS) + core
    partner = me + 1 - 2 * core
    chunks, rows = h1.shape[0], h1.shape[1]
    half = rows // 2
    quad = CHIPS * rows
    wide = 2 * quad
    vocab = lm_hbm.shape[0]
    model = hid.shape[-1]

    def block(b, lo, n):
        return pl.ds(pl.multiple_of((b % CHIPS) * rows + lo, half), n)

    def remote(src, dst, ssem, rsem, dev):
        return pltpu.make_async_remote_copy(src_ref=src, dst_ref=dst, send_sem=ssem, recv_sem=rsem,
                                            device_id={"tp": dev}, device_id_type=pl.DeviceIdType.MESH)

    barrier = pltpu.get_barrier_semaphore()
    for k in range(1, tp):
        pl.semaphore_signal(barrier, inc=1, device_id={"tp": (me + k) % tp}, device_id_type=pl.DeviceIdType.MESH)

    def token_rows(p, c):
        return pl.ds(pl.multiple_of(p * wide + c * quad, quad), quad)

    loads = []

    def load(src, dst):
        loads.append(pltpu.make_async_copy(src, dst, s_load.at[len(loads)]))
        loads[-1].start()

    for p in range(chunks):
        load(att_hbm.at[token_rows(p, core)], att_own.at[p])
    load(wo_hbm, wo.at[0])
    for p in range(chunks):
        load(hid_hbm.at[pl.ds(pl.multiple_of(p * wide + core * quad + x * rows, rows), rows)], hid.at[p])
    load(wg_hbm, wg.at[0])
    load(wu_hbm, wu.at[0])
    load(wd_hbm, wd.at[0])

    pl.semaphore_wait(barrier, tp - 1)

    pair = []
    for src, dst in ([(att_hbm.at[token_rows(p, 1 - core)], att_far.at[p]) for p in range(chunks)] +
                     [(wo_hbm, wo.at[1]), (wg_hbm, wg.at[1]), (wu_hbm, wu.at[1]), (wd_hbm, wd.at[1])]):
        pair.append(remote(src, dst, s_pair_s.at[len(pair)], s_pair_r.at[len(pair)], partner))
        pair[-1].start()

    full, rest = vocab // TILE, vocab % TILE
    count = full + (1 if rest else 0)

    def tile_copy(p, i, size):
        slot = (p * count + i) % 3
        start = i * TILE if isinstance(i, int) else pl.multiple_of(i * TILE, TILE)
        return pltpu.make_async_copy(lm_hbm.at[pl.ds(start, size)], tiles.at[slot, pl.ds(0, size)], s_tile.at[slot])

    def size_of(i):
        return TILE if i < full else rest

    tile_copy(0, 0, TILE).start()
    tile_copy(0, 1, TILE).start()

    def project(p):
        @pl.loop(0, model // COLS)
        def _(n):
            cols = pl.ds(pl.multiple_of(n * COLS, COLS), COLS)
            acc = jnp.dot(att_own[p], wo[0, :, cols], preferred_element_type=F32)
            acc = acc + jnp.dot(att_far[p], wo[1, :, cols], preferred_element_type=F32)
            part[0, p, :, cols] = acc.astype(BF16)

    def rs_copies(ph, p):
        mine = part.at[ph, p]
        sem = lambda k: (s_rs_s.at[ph, p, k], s_rs_r.at[ph, p, k])
        top, low = pl.ds(0, half), pl.ds(half, half)
        plan = [
            lambda: (mine.at[block(x + 2, 0, half)], mrg_in.at[ph, p, 0], *sem(0), right),
            lambda: (mine.at[block(x + 2, half, half)], mrg_in.at[ph, p, 1], *sem(1), left),
            lambda: (mine.at[block(x + 1, half, half)], fin_in.at[ph, p, 0, low], *sem(2), right),
            lambda: (mine.at[block(x + 3, 0, half)], fin_in.at[ph, p, 1, top], *sem(3), left),
            lambda: (mrg_out.at[ph, p, 0], fin_in.at[ph, p, 0, top], *sem(4), right),
            lambda: (mrg_out.at[ph, p, 1], fin_in.at[ph, p, 1, low], *sem(5), left),
        ]
        return Copies(remote, plan)

    def rs_start(ph, p):
        for k in range(4):
            rs_copies(ph, p)[k].start()

    def rs_merge(ph, p):
        c = rs_copies(ph, p)
        c[0].wait_recv()
        mrg_out[ph, p, 0] = (part[ph, p, block(x + 1, 0, half), :].astype(F32) + mrg_in[ph, p, 0].astype(F32)).astype(BF16)
        c[4].start()
        c[1].wait_recv()
        mrg_out[ph, p, 1] = (part[ph, p, block(x + 3, half, half), :].astype(F32) + mrg_in[ph, p, 1].astype(F32)).astype(BF16)
        c[5].start()

    def rs_finish(ph, p):
        c = rs_copies(ph, p)
        for k in (2, 3, 4, 5):
            c[k].wait_recv()
        total = part[ph, p, block(x, 0, rows), :].astype(F32) + fin_in[ph, p, 0].astype(F32) + fin_in[ph, p, 1].astype(F32)
        return total.astype(BF16).astype(F32)

    def ag_copies(ph, p):
        if ph == 0:
            at = lambda b, lo: gat.at[p, block(b, lo, half)]
        else:
            at = lambda b, lo: fin.at[p, pl.ds(pl.multiple_of(core * quad + (b % CHIPS) * rows + lo, half), half)]
        sem = lambda k: (s_ag_s.at[ph, p, k], s_ag_r.at[ph, p, k])
        plan = [(x, 0, right), (x, half, right), (x, half, left), (x, 0, left), (x + 3, 0, right), (x + 1, half, left)]
        return Copies(remote, [lambda k=k, b=b, lo=lo, dev=dev: (at(b, lo), at(b, lo), *sem(k), dev) for k, (b, lo, dev) in enumerate(plan)])

    def dd_copies(p):
        def plan(k):
            at = fin.at[p, pl.ds(pl.multiple_of(core * quad + ((x + k) % CHIPS) * rows, rows), rows)]
            return at, at, s_dd_s.at[p, k], s_dd_r.at[p, k], partner

        return Copies(remote, [functools.partial(plan, k) for k in range(CHIPS)])

    def ag_start(ph, p):
        c = ag_copies(ph, p)
        for k in (0, 2, 1, 3):
            c[k].start()
        if ph == 1:
            dd_copies(p)[0].start()

    def ag_forward(ph, p):
        c = ag_copies(ph, p)
        c[0].wait_recv()
        c[4].start()
        c[2].wait_recv()
        c[5].start()

    def ag_wait(ph, p):
        c = ag_copies(ph, p)
        d = dd_copies(p)
        c[1].wait_recv()
        if ph == 1:
            d[3].start()
        c[3].wait_recv()
        if ph == 1:
            d[1].start()
        c[4].wait_recv()
        c[5].wait_recv()
        if ph == 1:
            d[2].start()

    def dd_wait(p):
        for d in dd_copies(p).all():
            d.wait_recv()

    def attn_end(p):
        summed = rs_finish(0, p)
        res = (hid[p].astype(F32) + summed).astype(BF16)
        h1[p] = res
        gat[p, block(x, 0, rows), :] = rms_norm(res, gain_m[...])
        ag_start(0, p)

    def mlp_end(p):
        summed = rs_finish(1, p)
        res = (h1[p].astype(F32) + summed).astype(BF16)
        fin[p, pl.ds(pl.multiple_of(core * quad + x * rows, rows), rows), :] = rms_norm(res, gain_f[...])
        ag_start(1, p)

    def mlp(p):
        ffn = wg.shape[-1]
        for s in range(2):
            @pl.loop(0, ffn // COLS)
            def _(n):
                cols = pl.ds(pl.multiple_of(n * COLS, COLS), COLS)
                gate = jnp.dot(gat[p], wg[s, :, cols], preferred_element_type=F32)
                upper = jnp.dot(gat[p], wu[s, :, cols], preferred_element_type=F32)
                act[s, :, cols] = (jax.nn.silu(gate) * upper).astype(BF16)

        @pl.loop(0, model // COLS)
        def _(n):
            cols = pl.ds(pl.multiple_of(n * COLS, COLS), COLS)
            acc = jnp.dot(act[0], wd[0, :, cols], preferred_element_type=F32)
            acc = acc + jnp.dot(act[1], wd[1, :, cols], preferred_element_type=F32)
            part[1, p, :, cols] = acc.astype(BF16)

    def multiply(p, i, size, out):
        slot = (p * count + i) % 3
        tile_copy(p, i, size).wait()
        out[pl.ds(0, size), :] = lax.dot_general(tiles[slot, pl.ds(0, size), :], fin[p], (((1,), (1,)), ((), ())),
                                                 preferred_element_type=F32)

    def fold(p, i, size, src):
        goal = target[p] - (me * vocab + i * TILE) - lax.broadcasted_iota(jnp.int32, (8, wide), 0)
        depth = STEP // 8
        offsets = 8 * lax.broadcasted_iota(jnp.int32, (depth, 8, wide), 0)
        old = run[0]
        top = old
        for r in range(0, size, STEP):
            top = jnp.maximum(top, jnp.max(src[pl.ds(r, STEP), :].reshape(depth, 8, wide), axis=0))
        total = run[1] * jnp.exp(old - top)
        chosen = run[2]
        for r in range(0, size, STEP):
            piece = src[pl.ds(r, STEP), :].reshape(depth, 8, wide)
            total = total + jnp.sum(jnp.exp(piece - top[None]), axis=0)
            chosen = chosen + jnp.sum(jnp.where((goal - r)[None] == offsets, piece, 0.0), axis=0)
        run[0] = top
        run[1] = total
        run[2] = chosen

    def head(p, events):
        run[0] = jnp.full(run.shape[1:], -jnp.inf, F32)
        run[1] = jnp.zeros(run.shape[1:], F32)
        run[2] = jnp.zeros(run.shape[1:], F32)
        tile_copy(p, 2, TILE).start()
        multiply(p, 0, TILE, lga)

        def pairs(lo, hi):
            if lo >= hi:
                return

            @pl.loop(lo, hi)
            def _(j):
                i = 2 * j
                tile_copy(p, i + 3, TILE).start()
                multiply(p, i + 1, TILE, lgb)
                fold(p, i, TILE, lga)
                tile_copy(p, i + 4, TILE).start()
                multiply(p, i + 2, TILE, lga)
                fold(p, i + 1, TILE, lgb)

        loops = (full - 4) // 2
        cuts = sorted(set([0, loops] + [min(e[0], loops) for e in events]))
        for e in events:
            if e[0] == 0:
                e[1]()
        for lo, hi in zip(cuts[:-1], cuts[1:]):
            pairs(lo, hi)
            for e in events:
                if min(e[0], loops) == hi and e[0] > 0:
                    e[1]()
        done = 2 * loops
        bufs = (lga, lgb)
        for i in range(done, count):
            nxt = i + 3
            if nxt < count:
                tile_copy(p, nxt, size_of(nxt)).start()
            elif p + 1 < chunks and nxt - count < 2:
                tile_copy(p + 1, nxt - count, TILE).start()
            if i + 1 < count:
                multiply(p, i + 1, size_of(i + 1), bufs[(i + 1) % 2])
            fold(p, i, size_of(i), bufs[i % 2])
        top = jnp.max(run[0], axis=0, keepdims=True)
        total = jnp.sum(run[1] * jnp.exp(run[0] - top), axis=0, keepdims=True)
        chosen = jnp.sum(run[2], axis=0, keepdims=True)
        for k, row in enumerate((top, total, chosen)):
            for g in range(wide // 128):
                stats[me, k, pl.ds(p * (wide // 128) + g, 1), :] = row[:, g * 128:(g + 1) * 128]

    def wait_loads(lo, hi):
        for k in range(lo, hi):
            loads[k].wait()

    wait_loads(0, chunks + 1)
    for k in range(chunks):
        pair[k].wait_recv()
    pair[chunks].wait_recv()
    for p in range(chunks):
        project(p)
        rs_start(0, p)
    wait_loads(chunks + 1, 2 * chunks + 1)
    for p in range(chunks):
        rs_merge(0, p)
    attn_end(0)
    attn_end(1)
    ag_forward(0, 0)
    ag_forward(0, 1)
    wait_loads(2 * chunks + 1, len(loads))
    for k in (1, 2, 3):
        pair[chunks + k].wait_recv()
    for p in range(chunks):
        ag_wait(0, p)
        mlp(p)
        rs_start(1, p)
    rs_merge(1, 0)
    mlp_end(0)
    rs_merge(1, 1)
    mlp_end(1)
    ag_forward(1, 0)
    ag_wait(1, 0)
    dd_wait(0)
    head(0, [(2, lambda: ag_forward(1, 1)), (6, lambda: ag_wait(1, 1))])
    dd_wait(1)
    head(1, [])

    sent = []
    for k in range(1, tp):
        sent.append(remote(stats.at[me], stats.at[me], s_st_s.at[k - 1], s_st_r.at[k - 1], (me + k) % tp))
        sent[-1].start()
    for d in sent:
        d.wait_recv()
    top = stats[0, 0]
    for k in range(1, tp):
        top = jnp.maximum(top, stats[k, 0])
    total = jnp.zeros_like(top)
    chosen = jnp.zeros_like(top)
    for k in range(tp):
        total = total + stats[k, 1] * jnp.exp(stats[k, 0] - top)
        chosen = chosen + stats[k, 2]
    log_norm = top + jnp.log(total)
    norm_out[...] = log_norm
    prob_out[...] = chosen - log_norm

    for d in sent + pair:
        d.wait_send()
    for p in range(chunks):
        for ph in range(2):
            for d in rs_copies(ph, p).all() + ag_copies(ph, p).all():
                d.wait_send()
        for d in dd_copies(p).all():
            d.wait_send()


def tail(tp, attended, hidden, w_o, w_gate, w_up, w_down, w_lm, mlp_norm, final_norm, score_id):
    tokens, model = hidden.shape
    heads = attended.shape[-1]
    ffn = w_gate.shape[-1]
    rows = tokens // (CHUNKS * tp)
    quad = CHIPS * rows
    wide = 2 * quad
    target = jnp.broadcast_to(score_id.reshape(CHUNKS, 1, wide), (CHUNKS, 8, wide))
    anyspace = pl.BlockSpec(memory_space=pl.ANY)
    vmem = pl.BlockSpec(memory_space=pltpu.VMEM)
    dma = pltpu.SemaphoreType.DMA
    flops = 2 * tokens * model * (w_lm.shape[-1] + 3 * ffn + heads)
    log_norm, log_prob = pl.pallas_call(
        functools.partial(tail_body, tp),
        out_shape=[jax.ShapeDtypeStruct((tokens // 128, 128), F32)] * 2,
        in_specs=[anyspace] * 7 + [vmem] * 3,
        out_specs=[vmem] * 2,
        scratch_shapes=[
            pltpu.VMEM((CHUNKS, quad, heads), BF16), pltpu.VMEM((CHUNKS, quad, heads), BF16),
            pltpu.VMEM((CHUNKS, rows, model), BF16), pltpu.VMEM((2, heads, model), BF16),
            pltpu.VMEM((2, model, ffn), BF16), pltpu.VMEM((2, model, ffn), BF16), pltpu.VMEM((2, ffn, model), BF16),
            pltpu.VMEM((2, CHUNKS, quad, model), BF16), pltpu.VMEM((2, CHUNKS, 2, rows // 2, model), BF16),
            pltpu.VMEM((2, CHUNKS, 2, rows // 2, model), BF16), pltpu.VMEM((2, CHUNKS, 2, rows, model), BF16),
            pltpu.VMEM((CHUNKS, rows, model), BF16), pltpu.VMEM((CHUNKS, quad, model), BF16),
            pltpu.VMEM((CHUNKS, wide, model), BF16), pltpu.VMEM((2, quad, ffn), BF16),
            pltpu.VMEM((3, TILE, model), BF16), pltpu.VMEM((TILE, wide), F32), pltpu.VMEM((TILE, wide), F32),
            pltpu.VMEM((3, 8, wide), F32), pltpu.VMEM((tp, 3, tokens // 128, 128), F32),
            dma((2 * CHUNKS + 4,)), dma((CHUNKS + 4,)), dma((CHUNKS + 4,)),
            dma((2, CHUNKS, 6)), dma((2, CHUNKS, 6)), dma((2, CHUNKS, 6)), dma((2, CHUNKS, 6)),
            dma((CHUNKS, CHIPS)), dma((CHUNKS, CHIPS)), dma((3,)), dma((tp - 1,)), dma((tp - 1,)),
        ],
        compiler_params=pltpu.CompilerParams(collective_id=0, has_side_effects=True, vmem_limit_bytes=VMEM_LIMIT),
        cost_estimate=pl.CostEstimate(flops=flops, bytes_accessed=2 * CHUNKS * w_lm.size, transcendentals=tokens * w_lm.shape[-1]),
        name="layer_tail_and_head",
    )(attended, hidden, w_o, w_gate, w_up, w_down, w_lm.T, mlp_norm.reshape(1, -1), final_norm.reshape(1, -1), target)
    return log_norm, log_prob


def solution(mesh):
    tp = mesh.shape["tp"]

    def group_step(hidden, tree_mask, depth, ctx_len, block_table, score_id, k_cache, v_cache, attn_norm, w_q, w_k, w_v, w_o, mlp_norm, w_gate, w_up, w_down, final_norm, w_lm):
        requests, nodes, model = hidden.shape
        page_size, kv_local, head_dim = k_cache.shape[1:]
        span = block_table.shape[1] * page_size
        heads_local = w_q.shape[1] // head_dim
        normed = rms_norm(hidden, attn_norm)
        positions = ctx_len[:, None] + depth
        query = jnp.dot(normed, w_q, preferred_element_type=F32).reshape(requests, nodes, heads_local, head_dim)
        query = rotate(query, positions).astype(BF16).reshape(requests, nodes, kv_local, heads_local // kv_local, head_dim)
        key_new = jnp.dot(normed, w_k, preferred_element_type=F32).reshape(requests, nodes, kv_local, head_dim)
        key_new = rotate(key_new, positions).astype(BF16)
        val_new = jnp.dot(normed, w_v, preferred_element_type=F32).astype(BF16).reshape(requests, nodes, kv_local, head_dim)
        key_old = k_cache[block_table].reshape(requests, span, kv_local, head_dim)
        val_old = v_cache[block_table].reshape(requests, span, kv_local, head_dim)
        attended = tree_attention(query, key_new, val_new, key_old, val_old, tree_mask, ctx_len)
        attended = attended.reshape(requests * nodes, heads_local * head_dim)
        log_norm, log_prob = tail(tp, attended, hidden.reshape(requests * nodes, model), w_o, w_gate, w_up, w_down, w_lm, mlp_norm, final_norm, score_id)
        return (log_norm.reshape(requests, nodes), log_prob.reshape(requests, nodes),
                write_cache(k_cache, block_table, ctx_len, key_new), write_cache(v_cache, block_table, ctx_len, val_new))

    request_spec = P("dp", None, None)
    node_spec = P("dp", None)
    cache_spec = P("dp", None, "tp", None)
    shared_spec = P(None)
    column_spec = P(None, "tp")
    row_spec = P("tp", None)
    in_specs = (request_spec, request_spec, node_spec, P("dp"), node_spec, node_spec, cache_spec, cache_spec, shared_spec, column_spec, column_spec, column_spec, row_spec, shared_spec, column_spec, column_spec, row_spec, shared_spec, column_spec)
    out_specs = (node_spec, node_spec, cache_spec, cache_spec)
    return jax.shard_map(group_step, mesh=mesh, in_specs=in_specs, out_specs=out_specs, check_vma=False)
```

```python
import functools

import jax
import jax.numpy as jnp
from jax import lax
from jax.experimental import pallas as pl
from jax.experimental.pallas import tpu as pltpu
from jax.sharding import PartitionSpec as P

RMS_EPS = 1e-5
ROPE_THETA = 500000
CHIPS = 4
PER_STEP = 4
CHUNKS = 2
TILE = 512
COLS = 512
STEP = 32
VMEM_LIMIT = 67043328
F32 = jnp.float32
BF16 = jnp.bfloat16


def rms_norm(values, gain):
    widened = values.astype(F32)
    scale = lax.rsqrt(jnp.mean(widened * widened, axis=-1, keepdims=True) + RMS_EPS)
    return (widened * scale * gain.astype(F32)).astype(BF16)


def attention_body(per, pages, ctx, table, hidden, gain, w_q, w_k, w_v, cosine, sine, mask, k_in, v_in, att, k_out, v_out, w_kv, q_heads, k_old, v_old):
    step = pl.program_id(0)
    nodes = mask.shape[1]
    size = k_in.shape[1]
    dim = k_in.shape[2]
    heads = w_q.shape[1] // dim
    span = pages * size
    lanes = 2 * dim

    @pl.when(step == 0)
    def _():
        w_kv[pl.ds(0, dim), :] = w_k[...]
        w_kv[pl.ds(dim, dim), :] = w_v[...]
        k_out[...] = k_in[...]
        v_out[...] = v_in[...]

    normed = rms_norm(hidden[...], gain[...])
    queries = jnp.dot(normed, w_q[...], preferred_element_type=F32)
    pair = lax.dot_general(normed, w_kv[...], (((1,), (1,)), ((), ())), preferred_element_type=F32)
    lane = lax.broadcasted_iota(jnp.int32, (per * nodes, lanes), 1)
    lower = (lane % dim) < dim // 2

    def rotate(values):
        swapped = jnp.where(lower, pltpu.roll(values, lanes - dim // 2, 1), pltpu.roll(values, dim // 2, 1))
        return values * cosine[...] + swapped * sine[...]

    for h in range(0, heads, 2):
        turned = rotate(queries[:, h * dim:(h + 2) * dim]).astype(BF16)
        q_heads[h] = turned[:, :dim]
        q_heads[h + 1] = turned[:, dim:]
    pair = jnp.where(lane < dim, rotate(pair), pair).astype(BF16)
    scale = dim ** -0.5
    slot = lax.broadcasted_iota(jnp.int32, (heads * nodes, span), 1)
    row = lax.broadcasted_iota(jnp.int32, (size, dim), 0)
    for r in range(per):
        b = step * per + r
        length = ctx[b]
        for j in range(pages):
            page = table[b * pages + j]
            k_old[r, pl.ds(j * size, size), :] = k_in[page]
            v_old[r, pl.ds(j * size, size), :] = v_in[page]
        own = slice(r * nodes, (r + 1) * nodes)
        fresh = pair[own]
        k_new = fresh[:, :dim]
        v_new = fresh[:, dim:]
        query = q_heads[:, pl.ds(r * nodes, nodes), :].reshape(heads * nodes, dim)
        nt = (((1,), (1,)), ((), ()))
        score_old = lax.dot_general(query, k_old[r], nt, preferred_element_type=F32) * scale
        score_old = jnp.where(slot < length, score_old, -jnp.inf)
        score_new = lax.dot_general(query, k_new, nt, preferred_element_type=F32) * scale
        seen = jnp.broadcast_to((mask[r] > 0)[None], (heads, nodes, nodes)).reshape(heads * nodes, nodes)
        score_new = jnp.where(seen, score_new, -jnp.inf)
        top = jnp.maximum(jnp.max(score_old, axis=-1, keepdims=True), jnp.max(score_new, axis=-1, keepdims=True))
        prob_old = jnp.exp(score_old - top)
        prob_new = jnp.exp(score_new - top)
        total = jnp.sum(prob_old, axis=-1, keepdims=True) + jnp.sum(prob_new, axis=-1, keepdims=True)
        mixed = jnp.dot(prob_old.astype(BF16), v_old[r], preferred_element_type=F32)
        mixed = mixed + jnp.dot(prob_new.astype(BF16), v_new, preferred_element_type=F32)
        mixed = (mixed / total).astype(BF16)
        att[pl.ds(r * nodes, nodes), :] = jnp.concatenate([mixed[h * nodes:(h + 1) * nodes] for h in range(heads)], axis=-1)

        shift = length % size
        window = jnp.concatenate([fresh.astype(F32), jnp.zeros((size, lanes), F32)], axis=0)
        window = pltpu.roll(window, shift, 0)
        for j in range(nodes // size + 1):
            page = table[b * pages + jnp.minimum(length // size + j, pages - 1)]
            place = row + j * size
            fits = (place >= shift) & (place < shift + nodes)
            rows = window[j * size:(j + 1) * size]
            k_out[page] = jnp.where(fits, rows[:, :dim], k_out[page].astype(F32)).astype(BF16)
            v_out[page] = jnp.where(fits, rows[:, dim:], v_out[page].astype(F32)).astype(BF16)


def attention(hidden, tree_mask, depth, ctx_len, block_table, k_cache, v_cache, attn_norm, w_q, w_k, w_v):
    requests, nodes, model = hidden.shape
    blocks, size, kv_local, dim = k_cache.shape
    pages = block_table.shape[1]
    per = PER_STEP
    rows = per * nodes
    heads = w_q.shape[1] // dim
    half = dim // 2
    inv_freq = 1.0 / (ROPE_THETA ** (jnp.arange(half, dtype=F32) * (2.0 / dim)))
    angles = (ctx_len[:, None] + depth).astype(F32).reshape(requests * nodes, 1) * jnp.tile(inv_freq, 4)[None, :]
    cosine = jnp.cos(angles)
    sine = jnp.sin(angles) * jnp.tile(jnp.repeat(jnp.array([-1.0, 1.0], F32), half), 2)[None, :]
    whole = lambda *shape: pl.BlockSpec(shape, lambda i, *_: (0,) * len(shape))
    by_row = lambda width: pl.BlockSpec((rows, width), lambda i, *_: (i, 0))
    cache_type = jax.ShapeDtypeStruct((blocks, size, dim), BF16)
    att, k_out, v_out = pl.pallas_call(
        functools.partial(attention_body, per, pages),
        out_shape=[jax.ShapeDtypeStruct((requests * nodes, heads * dim), BF16), cache_type, cache_type],
        grid_spec=pltpu.PrefetchScalarGridSpec(
            num_scalar_prefetch=2,
            grid=(requests // per,),
            in_specs=[by_row(model), whole(1, model), whole(model, heads * dim), whole(dim, model), whole(dim, model),
                      by_row(2 * dim), by_row(2 * dim), pl.BlockSpec((per, nodes, nodes), lambda i, *_: (i, 0, 0)),
                      whole(blocks, size, dim), whole(blocks, size, dim)],
            out_specs=[by_row(heads * dim), whole(blocks, size, dim), whole(blocks, size, dim)],
            scratch_shapes=[pltpu.VMEM((2 * dim, model), BF16), pltpu.VMEM((heads, rows, dim), BF16),
                            pltpu.VMEM((per, pages * size, dim), BF16), pltpu.VMEM((per, pages * size, dim), BF16)],
        ),
        compiler_params=pltpu.CompilerParams(vmem_limit_bytes=48 * 1024 * 1024),
        cost_estimate=pl.CostEstimate(flops=2 * requests * nodes * model * (heads + 2) * dim, bytes_accessed=hidden.size * 2, transcendentals=0),
        name="tree_attention",
    )(ctx_len, block_table.reshape(-1), hidden.reshape(requests * nodes, model), attn_norm.reshape(1, -1), w_q, w_k.T, w_v.T,
      cosine, sine, tree_mask, k_cache.reshape(blocks, size, dim), v_cache.reshape(blocks, size, dim))
    return att, k_out.reshape(k_cache.shape), v_out.reshape(v_cache.shape)


class Copies:
    def __init__(self, make, plan):
        self.make = make
        self.plan = plan

    def __getitem__(self, k):
        return self.make(*self.plan[k]())

    def all(self):
        return [self[k] for k in range(len(self.plan))]


def tail_body(tp, att_hbm, hid_hbm, wo_hbm, wg_hbm, wu_hbm, wd_hbm, lm_hbm, gain_m, gain_f, target, norm_out, prob_out,
              att_own, att_far, hid, wo, wg, wu, wd, part, mrg_in, mrg_out, fin_in, h1, gat, fin, act, tiles, lga, lgb, run, stats,
              s_load, s_pair_s, s_pair_r, s_rs_s, s_rs_r, s_ag_s, s_ag_r, s_dd_s, s_dd_r, s_tile, s_st_s, s_st_r):
    me = lax.axis_index("tp")
    x = me // 2
    core = me % 2
    right = 2 * ((x + 1) % CHIPS) + core
    left = 2 * ((x + CHIPS - 1) % CHIPS) + core
    partner = me + 1 - 2 * core
    chunks, rows = h1.shape[0], h1.shape[1]
    half = rows // 2
    quad = CHIPS * rows
    wide = 2 * quad
    vocab = lm_hbm.shape[0]
    model = hid.shape[-1]

    def block(b, lo, n):
        return pl.ds(pl.multiple_of((b % CHIPS) * rows + lo, half), n)

    def remote(src, dst, ssem, rsem, dev):
        return pltpu.make_async_remote_copy(src_ref=src, dst_ref=dst, send_sem=ssem, recv_sem=rsem,
                                            device_id={"tp": dev}, device_id_type=pl.DeviceIdType.MESH)

    barrier = pltpu.get_barrier_semaphore()
    for k in range(1, tp):
        pl.semaphore_signal(barrier, inc=1, device_id={"tp": (me + k) % tp}, device_id_type=pl.DeviceIdType.MESH)

    def token_rows(p, c):
        return pl.ds(pl.multiple_of(p * wide + c * quad, quad), quad)

    loads = []

    def load(src, dst):
        loads.append(pltpu.make_async_copy(src, dst, s_load.at[len(loads)]))
        loads[-1].start()

    for p in range(chunks):
        load(att_hbm.at[token_rows(p, core)], att_own.at[p])
    load(wo_hbm, wo.at[0])
    for p in range(chunks):
        load(hid_hbm.at[pl.ds(pl.multiple_of(p * wide + core * quad + x * rows, rows), rows)], hid.at[p])
    load(wg_hbm, wg.at[0])
    load(wu_hbm, wu.at[0])
    load(wd_hbm, wd.at[0])

    pl.semaphore_wait(barrier, tp - 1)

    pair = []
    for src, dst in ([(att_hbm.at[token_rows(p, 1 - core)], att_far.at[p]) for p in range(chunks)] +
                     [(wo_hbm, wo.at[1]), (wg_hbm, wg.at[1]), (wu_hbm, wu.at[1]), (wd_hbm, wd.at[1])]):
        pair.append(remote(src, dst, s_pair_s.at[len(pair)], s_pair_r.at[len(pair)], partner))
        pair[-1].start()

    full, rest = vocab // TILE, vocab % TILE
    count = full + 1
    assert full % 2 == 1 and rest % STEP == 0 and rest > 0

    def tile_copy(p, i, size):
        slot = (p * count + i) % 3
        start = i * TILE if isinstance(i, int) else pl.multiple_of(i * TILE, TILE)
        return pltpu.make_async_copy(lm_hbm.at[pl.ds(start, size)], tiles.at[slot, pl.ds(0, size)], s_tile.at[slot])

    tile_copy(0, 0, TILE).start()
    tile_copy(0, 1, TILE).start()

    def project(p):
        @pl.loop(0, model // COLS)
        def _(n):
            cols = pl.ds(pl.multiple_of(n * COLS, COLS), COLS)
            acc = jnp.dot(att_own[p], wo[0, :, cols], preferred_element_type=F32)
            acc = acc + jnp.dot(att_far[p], wo[1, :, cols], preferred_element_type=F32)
            part[0, p, :, cols] = acc.astype(BF16)

    def rs_copies(ph, p):
        mine = part.at[ph, p]
        sem = lambda k: (s_rs_s.at[ph, p, k], s_rs_r.at[ph, p, k])
        top, low = pl.ds(0, half), pl.ds(half, half)
        plan = [
            lambda: (mine.at[block(x + 2, 0, half)], mrg_in.at[ph, p, 0], *sem(0), right),
            lambda: (mine.at[block(x + 2, half, half)], mrg_in.at[ph, p, 1], *sem(1), left),
            lambda: (mine.at[block(x + 1, half, half)], fin_in.at[ph, p, 0, low], *sem(2), right),
            lambda: (mine.at[block(x + 3, 0, half)], fin_in.at[ph, p, 1, top], *sem(3), left),
            lambda: (mrg_out.at[ph, p, 0], fin_in.at[ph, p, 0, top], *sem(4), right),
            lambda: (mrg_out.at[ph, p, 1], fin_in.at[ph, p, 1, low], *sem(5), left),
        ]
        return Copies(remote, plan)

    def rs_start(ph, p):
        for k in range(4):
            rs_copies(ph, p)[k].start()

    def rs_merge(ph, p):
        c = rs_copies(ph, p)
        c[0].wait_recv()
        mrg_out[ph, p, 0] = (part[ph, p, block(x + 1, 0, half), :].astype(F32) + mrg_in[ph, p, 0].astype(F32)).astype(BF16)
        c[4].start()
        c[1].wait_recv()
        mrg_out[ph, p, 1] = (part[ph, p, block(x + 3, half, half), :].astype(F32) + mrg_in[ph, p, 1].astype(F32)).astype(BF16)
        c[5].start()

    def rs_finish(ph, p):
        c = rs_copies(ph, p)
        for k in (2, 3, 4, 5):
            c[k].wait_recv()
        total = part[ph, p, block(x, 0, rows), :].astype(F32) + fin_in[ph, p, 0].astype(F32) + fin_in[ph, p, 1].astype(F32)
        return total.astype(BF16).astype(F32)

    def ag_copies(ph, p):
        if ph == 0:
            at = lambda b, lo: gat.at[p, block(b, lo, half)]
        else:
            at = lambda b, lo: fin.at[p, pl.ds(pl.multiple_of(core * quad + (b % CHIPS) * rows + lo, half), half)]
        sem = lambda k: (s_ag_s.at[ph, p, k], s_ag_r.at[ph, p, k])
        plan = [(x, 0, right), (x, half, right), (x, half, left), (x, 0, left), (x + 3, 0, right), (x + 1, half, left)]
        return Copies(remote, [lambda k=k, b=b, lo=lo, dev=dev: (at(b, lo), at(b, lo), *sem(k), dev) for k, (b, lo, dev) in enumerate(plan)])

    def dd_copies(p):
        def plan(k):
            at = fin.at[p, pl.ds(pl.multiple_of(core * quad + ((x + k) % CHIPS) * rows, rows), rows)]
            return at, at, s_dd_s.at[p, k], s_dd_r.at[p, k], partner

        return Copies(remote, [functools.partial(plan, k) for k in range(CHIPS)])

    def ag_start(ph, p):
        c = ag_copies(ph, p)
        for k in (0, 2, 1, 3):
            c[k].start()
        if ph == 1:
            dd_copies(p)[0].start()

    def ag_forward(ph, p):
        c = ag_copies(ph, p)
        c[0].wait_recv()
        c[4].start()
        c[2].wait_recv()
        c[5].start()

    def ag_wait(ph, p):
        c = ag_copies(ph, p)
        d = dd_copies(p)
        c[1].wait_recv()
        if ph == 1:
            d[3].start()
        c[3].wait_recv()
        if ph == 1:
            d[1].start()
        c[4].wait_recv()
        c[5].wait_recv()
        if ph == 1:
            d[2].start()

    def dd_wait(p):
        for d in dd_copies(p).all():
            d.wait_recv()

    def attn_end(p):
        summed = rs_finish(0, p)
        res = (hid[p].astype(F32) + summed).astype(BF16)
        h1[p] = res
        gat[p, block(x, 0, rows), :] = rms_norm(res, gain_m[...])
        ag_start(0, p)

    def mlp_end(p):
        summed = rs_finish(1, p)
        res = (h1[p].astype(F32) + summed).astype(BF16)
        fin[p, pl.ds(pl.multiple_of(core * quad + x * rows, rows), rows), :] = rms_norm(res, gain_f[...])
        ag_start(1, p)

    def mlp(p, between=None):
        ffn = wg.shape[-1]
        for s in range(2):
            @pl.loop(0, ffn // COLS)
            def _(n):
                cols = pl.ds(pl.multiple_of(n * COLS, COLS), COLS)
                gate = jnp.dot(gat[p], wg[s, :, cols], preferred_element_type=F32)
                upper = jnp.dot(gat[p], wu[s, :, cols], preferred_element_type=F32)
                act[s, :, cols] = (jax.nn.silu(gate) * upper).astype(BF16)

            if s == 0 and between is not None:
                between()

        @pl.loop(0, model // COLS)
        def _(n):
            cols = pl.ds(pl.multiple_of(n * COLS, COLS), COLS)
            acc = jnp.dot(act[0], wd[0, :, cols], preferred_element_type=F32)
            acc = acc + jnp.dot(act[1], wd[1, :, cols], preferred_element_type=F32)
            part[1, p, :, cols] = acc.astype(BF16)

    def multiply(p, i, size, out):
        slot = (p * count + i) % 3
        tile_copy(p, i, size).wait()
        out[pl.ds(0, size), :] = lax.dot_general(tiles[slot, pl.ds(0, size), :], fin[p], (((1,), (1,)), ((), ())),
                                                 preferred_element_type=F32)

    def fold(p, i, size, src):
        goal = target[p] - (me * vocab + i * TILE) - lax.broadcasted_iota(jnp.int32, (8, wide), 0)
        depth = STEP // 8
        offsets = 8 * lax.broadcasted_iota(jnp.int32, (depth, 8, wide), 0)
        old = run[0]
        top = old
        for r in range(0, size, STEP):
            top = jnp.maximum(top, jnp.max(src[pl.ds(r, STEP), :].reshape(depth, 8, wide), axis=0))
        total = run[1] * jnp.exp(old - top)
        chosen = run[2]
        for r in range(0, size, STEP):
            piece = src[pl.ds(r, STEP), :].reshape(depth, 8, wide)
            total = total + jnp.sum(jnp.exp(piece - top[None]), axis=0)
            chosen = chosen + jnp.sum(jnp.where((goal - r)[None] == offsets, piece, 0.0), axis=0)
        run[0] = top
        run[1] = total
        run[2] = chosen

    def prefetch(p, i):
        @pl.when(i < full)
        def _():
            tile_copy(p, i, TILE).start()

        @pl.when(i == full)
        def _():
            tile_copy(p, full, rest).start()

    def head(p, events):
        run[0] = jnp.full(run.shape[1:], -jnp.inf, F32)
        run[1] = jnp.zeros(run.shape[1:], F32)
        run[2] = jnp.zeros(run.shape[1:], F32)
        tile_copy(p, 2, TILE).start()
        multiply(p, 0, TILE, lga)

        @pl.loop(0, full // 2)
        def _(j):
            for when, event in events:
                pl.when(j == when)(event)
            i = 2 * j
            prefetch(p, i + 3)
            multiply(p, i + 1, TILE, lgb)
            fold(p, i, TILE, lga)
            prefetch(p, i + 4)
            multiply(p, i + 2, TILE, lga)
            fold(p, i + 1, TILE, lgb)

        if p + 1 < chunks:
            tile_copy(p + 1, 0, TILE).start()
            tile_copy(p + 1, 1, TILE).start()
        multiply(p, full, rest, lgb)
        fold(p, full - 1, TILE, lga)
        fold(p, full, rest, lgb)
        top = jnp.max(run[0], axis=0, keepdims=True)
        total = jnp.sum(run[1] * jnp.exp(run[0] - top), axis=0, keepdims=True)
        chosen = jnp.sum(run[2], axis=0, keepdims=True)
        for k, row in enumerate((top, total, chosen)):
            for g in range(wide // 128):
                stats[me, k, pl.ds(p * (wide // 128) + g, 1), :] = row[:, g * 128:(g + 1) * 128]

    def wait_loads(lo, hi):
        for k in range(lo, hi):
            loads[k].wait()

    wait_loads(0, chunks + 1)
    for k in range(chunks):
        pair[k].wait_recv()
    pair[chunks].wait_recv()
    project(0)
    rs_start(0, 0)
    wait_loads(chunks + 1, 2 * chunks + 1)
    project(1)
    rs_merge(0, 0)
    attn_end(0)
    ag_forward(0, 0)
    rs_start(0, 1)
    wait_loads(2 * chunks + 1, len(loads))
    for k in (1, 2, 3):
        pair[chunks + k].wait_recv()
    ag_wait(0, 0)
    mlp(0, lambda: rs_merge(0, 1))
    rs_start(1, 0)
    rs_merge(1, 0)
    mlp_end(0)
    ag_forward(1, 0)
    attn_end(1)
    ag_wait(1, 0)
    dd_wait(0)

    def second_mlp():
        ag_wait(0, 1)
        mlp(1)
        rs_start(1, 1)

    head(0, [(1, lambda: ag_forward(0, 1)), (3, second_mlp), (5, lambda: rs_merge(1, 1)), (7, lambda: mlp_end(1)),
             (9, lambda: ag_forward(1, 1)), (11, lambda: ag_wait(1, 1))])
    dd_wait(1)
    head(1, [])

    sent = []
    for k in range(1, tp):
        sent.append(remote(stats.at[me], stats.at[me], s_st_s.at[k - 1], s_st_r.at[k - 1], (me + k) % tp))
        sent[-1].start()
    for d in sent:
        d.wait_recv()
    top = stats[0, 0]
    for k in range(1, tp):
        top = jnp.maximum(top, stats[k, 0])
    total = jnp.zeros_like(top)
    chosen = jnp.zeros_like(top)
    for k in range(tp):
        total = total + stats[k, 1] * jnp.exp(stats[k, 0] - top)
        chosen = chosen + stats[k, 2]
    log_norm = top + jnp.log(total)
    norm_out[...] = log_norm
    prob_out[...] = chosen - log_norm

    for d in sent + pair:
        d.wait_send()
    for p in range(chunks):
        for ph in range(2):
            for d in rs_copies(ph, p).all() + ag_copies(ph, p).all():
                d.wait_send()
        for d in dd_copies(p).all():
            d.wait_send()


def tail(tp, attended, hidden, w_o, w_gate, w_up, w_down, w_lm, mlp_norm, final_norm, score_id):
    tokens, model = hidden.shape
    heads = attended.shape[-1]
    ffn = w_gate.shape[-1]
    rows = tokens // (CHUNKS * tp)
    quad = CHIPS * rows
    wide = 2 * quad
    target = jnp.broadcast_to(score_id.reshape(CHUNKS, 1, wide), (CHUNKS, 8, wide))
    anyspace = pl.BlockSpec(memory_space=pl.ANY)
    vmem = pl.BlockSpec(memory_space=pltpu.VMEM)
    dma = pltpu.SemaphoreType.DMA
    flops = 2 * tokens * model * (w_lm.shape[-1] + 3 * ffn + heads)
    log_norm, log_prob = pl.pallas_call(
        functools.partial(tail_body, tp),
        out_shape=[jax.ShapeDtypeStruct((tokens // 128, 128), F32)] * 2,
        in_specs=[anyspace] * 7 + [vmem] * 3,
        out_specs=[vmem] * 2,
        scratch_shapes=[
            pltpu.VMEM((CHUNKS, quad, heads), BF16), pltpu.VMEM((CHUNKS, quad, heads), BF16),
            pltpu.VMEM((CHUNKS, rows, model), BF16), pltpu.VMEM((2, heads, model), BF16),
            pltpu.VMEM((2, model, ffn), BF16), pltpu.VMEM((2, model, ffn), BF16), pltpu.VMEM((2, ffn, model), BF16),
            pltpu.VMEM((2, CHUNKS, quad, model), BF16), pltpu.VMEM((2, CHUNKS, 2, rows // 2, model), BF16),
            pltpu.VMEM((2, CHUNKS, 2, rows // 2, model), BF16), pltpu.VMEM((2, CHUNKS, 2, rows, model), BF16),
            pltpu.VMEM((CHUNKS, rows, model), BF16), pltpu.VMEM((CHUNKS, quad, model), BF16),
            pltpu.VMEM((CHUNKS, wide, model), BF16), pltpu.VMEM((2, quad, ffn), BF16),
            pltpu.VMEM((3, TILE, model), BF16), pltpu.VMEM((TILE, wide), F32), pltpu.VMEM((TILE, wide), F32),
            pltpu.VMEM((3, 8, wide), F32), pltpu.VMEM((tp, 3, tokens // 128, 128), F32),
            dma((2 * CHUNKS + 4,)), dma((CHUNKS + 4,)), dma((CHUNKS + 4,)),
            dma((2, CHUNKS, 6)), dma((2, CHUNKS, 6)), dma((2, CHUNKS, 6)), dma((2, CHUNKS, 6)),
            dma((CHUNKS, CHIPS)), dma((CHUNKS, CHIPS)), dma((3,)), dma((tp - 1,)), dma((tp - 1,)),
        ],
        compiler_params=pltpu.CompilerParams(collective_id=0, has_side_effects=True, vmem_limit_bytes=VMEM_LIMIT),
        cost_estimate=pl.CostEstimate(flops=flops, bytes_accessed=2 * CHUNKS * w_lm.size, transcendentals=tokens * w_lm.shape[-1]),
        name="layer_tail_and_head",
    )(attended, hidden, w_o, w_gate, w_up, w_down, w_lm.T, mlp_norm.reshape(1, -1), final_norm.reshape(1, -1), target)
    return log_norm, log_prob


def solution(mesh):
    tp = mesh.shape["tp"]

    def group_step(hidden, tree_mask, depth, ctx_len, block_table, score_id, k_cache, v_cache, attn_norm, w_q, w_k, w_v, w_o, mlp_norm, w_gate, w_up, w_down, final_norm, w_lm):
        requests, nodes, model = hidden.shape
        attended, k_out, v_out = attention(hidden, tree_mask, depth, ctx_len, block_table, k_cache, v_cache, attn_norm, w_q, w_k, w_v)
        log_norm, log_prob = tail(tp, attended, hidden.reshape(requests * nodes, model), w_o, w_gate, w_up, w_down, w_lm, mlp_norm, final_norm, score_id)
        return log_norm.reshape(requests, nodes), log_prob.reshape(requests, nodes), k_out, v_out

    request_spec = P("dp", None, None)
    node_spec = P("dp", None)
    cache_spec = P("dp", None, "tp", None)
    shared_spec = P(None)
    column_spec = P(None, "tp")
    row_spec = P("tp", None)
    in_specs = (request_spec, request_spec, node_spec, P("dp"), node_spec, node_spec, cache_spec, cache_spec, shared_spec, column_spec, column_spec, column_spec, row_spec, shared_spec, column_spec, column_spec, row_spec, shared_spec, column_spec)
    out_specs = (node_spec, node_spec, cache_spec, cache_spec)
    return jax.shard_map(group_step, mesh=mesh, in_specs=in_specs, out_specs=out_specs, check_vma=False)
```

```python
import functools

import jax
import jax.numpy as jnp
from jax import lax
from jax.experimental import pallas as pl
from jax.experimental.pallas import tpu as pltpu
from jax.sharding import PartitionSpec as P

RMS_EPS = 1e-5
ROPE_THETA = 500000
CHIPS = 4
PER_STEP = 4
SHARES = (1, 1, 2)
TILE = 1024
COLS = 512
STEP = 32
VMEM_LIMIT = 67043328
F32 = jnp.float32
BF16 = jnp.bfloat16


def rms_norm(values, gain):
    widened = values.astype(F32)
    scale = lax.rsqrt(jnp.mean(widened * widened, axis=-1, keepdims=True) + RMS_EPS)
    return (widened * scale * gain.astype(F32)).astype(BF16)


def attention_body(per, pages, ctx, table, hidden, gain, w_q, w_k, w_v, cosine, sine, mask, k_in, v_in, att, k_out, v_out, w_kv, q_heads, kv_old, kv):
    step = pl.program_id(0)
    nodes = mask.shape[1]
    size, dim, blocks = k_in.shape
    lanes = 2 * dim
    pitch = kv.shape[0] // size
    heads = w_q.shape[1] // dim
    span = pages * size

    @pl.when(step == 0)
    def _():
        w_kv[pl.ds(0, dim), :] = w_k[...]
        w_kv[pl.ds(dim, dim), :] = w_v[...]
        for s in range(size):
            joined = jnp.concatenate([k_in[s].astype(F32), v_in[s].astype(F32)], axis=0)
            kv[pl.ds(s * pitch, blocks), :] = joined.T

    normed = rms_norm(hidden[...], gain[...].reshape(1, -1))
    nt = (((1,), (1,)), ((), ()))
    queries = jnp.dot(normed, w_q[...], preferred_element_type=F32)
    pair = lax.dot_general(normed, w_kv[...], nt, preferred_element_type=F32)
    lane = lax.broadcasted_iota(jnp.int32, (per * nodes, lanes), 1)
    lower = (lane % dim) < dim // 2

    def rotate(values):
        swapped = jnp.where(lower, pltpu.roll(values, lanes - dim // 2, 1), pltpu.roll(values, dim // 2, 1))
        return values * cosine[...] + swapped * sine[...]

    for h in range(0, heads, 2):
        turned = rotate(queries[:, h * dim:(h + 2) * dim])
        q_heads[h] = jnp.where(lane < dim, turned, 0.0).astype(BF16)
        q_heads[h + 1] = jnp.where(lane < dim, pltpu.roll(turned, dim, 1), 0.0).astype(BF16)
    pair = jnp.where(lane < dim, rotate(pair), pair).astype(BF16)
    scale = dim ** -0.5
    slot = lax.broadcasted_iota(jnp.int32, (heads * nodes, span), 1)
    row = lax.broadcasted_iota(jnp.int32, (size, lanes), 0)
    for r in range(per):
        b = step * per + r
        length = ctx[b]
        for j in range(pages):
            kv_old[r, pl.ds(j * size, size), :] = kv[pl.ds(table[b, j], size, stride=pitch), :].astype(BF16)
        fresh = pair[r * nodes:(r + 1) * nodes]
        query = q_heads[:, pl.ds(r * nodes, nodes), :].reshape(heads * nodes, lanes)
        score_old = lax.dot_general(query, kv_old[r], nt, preferred_element_type=F32) * scale
        score_old = jnp.where(slot < length, score_old, -jnp.inf)
        score_new = lax.dot_general(query, fresh, nt, preferred_element_type=F32) * scale
        seen = jnp.broadcast_to((mask[r] > 0)[None], (heads, nodes, nodes)).reshape(heads * nodes, nodes)
        score_new = jnp.where(seen, score_new, -jnp.inf)
        top = jnp.maximum(jnp.max(score_old, axis=-1, keepdims=True), jnp.max(score_new, axis=-1, keepdims=True))
        prob_old = jnp.exp(score_old - top)
        prob_new = jnp.exp(score_new - top)
        total = jnp.sum(prob_old, axis=-1, keepdims=True) + jnp.sum(prob_new, axis=-1, keepdims=True)
        mixed = jnp.dot(prob_old.astype(BF16), kv_old[r], preferred_element_type=F32)
        mixed = mixed + jnp.dot(prob_new.astype(BF16), fresh, preferred_element_type=F32)
        mixed = mixed / total
        for h in range(0, heads, 2):
            even = pltpu.roll(mixed[h * nodes:(h + 1) * nodes], dim, 1)
            odd = mixed[(h + 1) * nodes:(h + 2) * nodes]
            joined = jnp.where(lane[:nodes] < dim, even, odd)
            att[pl.ds(r * nodes, nodes), h * dim:(h + 2) * dim] = joined.astype(BF16)

        shift = length % size
        window = jnp.concatenate([fresh.astype(F32), jnp.zeros((size, lanes), F32)], axis=0)
        window = pltpu.roll(window, shift, 0)
        for j in range(nodes // size + 1):
            page = table[b, jnp.minimum(length // size + j, pages - 1)]
            place = row + j * size
            fits = (place >= shift) & (place < shift + nodes)
            at = pl.ds(page, size, stride=pitch)
            kv[at, :] = jnp.where(fits, window[j * size:(j + 1) * size], kv[at, :])

    @pl.when(step == pl.num_programs(0) - 1)
    def _():
        for s in range(size):
            apart = kv[pl.ds(s * pitch, blocks), :].T.astype(BF16)
            k_out[s] = apart[:dim]
            v_out[s] = apart[dim:]


def attention(hidden, tree_mask, depth, ctx_len, block_table, k_cache, v_cache, attn_norm, w_q, w_k, w_v):
    requests, nodes, model = hidden.shape
    blocks, size, kv_local, dim = k_cache.shape
    pages = block_table.shape[1]
    per = PER_STEP
    rows = per * nodes
    heads = w_q.shape[1] // dim
    half = dim // 2
    lane = jnp.arange(2 * dim)
    inv_freq = 1.0 / (ROPE_THETA ** ((lane % half).astype(F32) * (2.0 / dim)))
    angles = (ctx_len[:, None] + depth).astype(F32)[..., None] * inv_freq
    cosine = jnp.cos(angles).reshape(requests * nodes, 2 * dim)
    sine = (jnp.sin(angles) * jnp.where(lane % dim < half, -1.0, 1.0)).reshape(requests * nodes, 2 * dim)
    stored = lambda cache: cache.transpose(1, 2, 3, 0).reshape(size, dim, blocks)
    native = lambda cache: cache.reshape(size, kv_local, dim, blocks).transpose(3, 0, 1, 2)
    cache_type = jax.ShapeDtypeStruct((size, dim, blocks), BF16)
    whole = lambda *shape: pl.BlockSpec(shape, lambda i, *_: (0,) * len(shape))
    by_row = lambda width: pl.BlockSpec((rows, width), lambda i, *_: (i, 0))
    att, k_out, v_out = pl.pallas_call(
        functools.partial(attention_body, per, pages),
        out_shape=[jax.ShapeDtypeStruct((requests * nodes, heads * dim), BF16), cache_type, cache_type],
        grid_spec=pltpu.PrefetchScalarGridSpec(
            num_scalar_prefetch=2,
            grid=(requests // per,),
            in_specs=[by_row(model), whole(model), whole(model, heads * dim), whole(dim, model), whole(dim, model),
                      by_row(2 * dim), by_row(2 * dim), pl.BlockSpec((per, nodes, nodes), lambda i, *_: (i, 0, 0)),
                      whole(size, dim, blocks), whole(size, dim, blocks)],
            out_specs=[by_row(heads * dim), whole(size, dim, blocks), whole(size, dim, blocks)],
            scratch_shapes=[pltpu.VMEM((2 * dim, model), BF16), pltpu.VMEM((heads, rows, 2 * dim), BF16),
                            pltpu.VMEM((per, pages * size, 2 * dim), BF16), pltpu.VMEM((size * (blocks + 8), 2 * dim), F32)],
        ),
        compiler_params=pltpu.CompilerParams(vmem_limit_bytes=VMEM_LIMIT),
        cost_estimate=pl.CostEstimate(flops=2 * requests * nodes * model * (heads + 2) * dim, bytes_accessed=hidden.size * 2, transcendentals=0),
        name="tree_attention",
    )(ctx_len, block_table, hidden.reshape(requests * nodes, model), attn_norm, w_q, w_k.T, w_v.T,
      cosine, sine, tree_mask, stored(k_cache), stored(v_cache))
    return att, native(k_out), native(v_out)


class Copies:
    def __init__(self, make, plan):
        self.make = make
        self.plan = plan

    def __getitem__(self, k):
        return self.make(*self.plan[k]())

    def all(self):
        return [self[k] for k in range(len(self.plan))]


def tail_body(tp, att_hbm, hid_hbm, wo_hbm, wg_hbm, wu_hbm, wd_hbm, lm_hbm, gain_m, gain_f, target, norm_out, prob_out,
              att_own, att_far, hid, wo, wg, wu, wd, part, mrg_in, mrg_out, fin_in, h1, gat, fin, act, tiles, lga, lgb, run, stats,
              s_load, s_pair_s, s_pair_r, s_rs_s, s_rs_r, s_ag_s, s_ag_r, s_dd_s, s_dd_r, s_tile, s_st_s, s_st_r):
    me = lax.axis_index("tp")
    x = me // 2
    core = me % 2
    right = 2 * ((x + 1) % CHIPS) + core
    left = 2 * ((x + CHIPS - 1) % CHIPS) + core
    partner = me + 1 - 2 * core
    chunks = len(SHARES)
    rows = [h1.shape[0] * share // sum(SHARES) for share in SHARES]
    base = [sum(rows[:p]) for p in range(chunks)]
    vocab = lm_hbm.shape[0]
    model = hid.shape[-1]

    def own(p):
        return pl.ds(base[p], rows[p])

    def quad(p):
        return pl.ds(CHIPS * base[p], CHIPS * rows[p])

    def wide(p):
        return pl.ds(2 * CHIPS * base[p], 2 * CHIPS * rows[p])

    def front(p):
        return pl.ds(base[p] // 2, rows[p] // 2)

    def block(p, b, lo, n):
        return pl.ds(pl.multiple_of(CHIPS * base[p] + (b % CHIPS) * rows[p] + lo, rows[p] // 2), n)

    def placed(p, b, lo, n):
        return pl.ds(pl.multiple_of(CHIPS * (2 * base[p] + core * rows[p]) + (b % CHIPS) * rows[p] + lo, rows[p] // 2), n)

    def remote(src, dst, ssem, rsem, dev):
        return pltpu.make_async_remote_copy(src_ref=src, dst_ref=dst, send_sem=ssem, recv_sem=rsem,
                                            device_id={"tp": dev}, device_id_type=pl.DeviceIdType.MESH)

    barrier = pltpu.get_barrier_semaphore()
    for k in range(1, tp):
        pl.semaphore_signal(barrier, inc=1, device_id={"tp": (me + k) % tp}, device_id_type=pl.DeviceIdType.MESH)

    def token_rows(p, c):
        return pl.ds(pl.multiple_of(CHIPS * (2 * base[p] + c * rows[p]), CHIPS * rows[p]), CHIPS * rows[p])

    loads = []

    def load(src, dst):
        loads.append(pltpu.make_async_copy(src, dst, s_load.at[len(loads)]))
        loads[-1].start()

    for p in range(chunks):
        load(att_hbm.at[token_rows(p, core)], att_own.at[quad(p)])
    load(wo_hbm, wo.at[0])
    for p in range(chunks):
        load(hid_hbm.at[placed(p, x, 0, rows[p])], hid.at[own(p)])
    load(wg_hbm, wg.at[0])
    load(wu_hbm, wu.at[0])
    load(wd_hbm, wd.at[0])

    pl.semaphore_wait(barrier, tp - 1)

    pair = []
    for src, dst in ([(att_hbm.at[token_rows(p, 1 - core)], att_far.at[quad(p)]) for p in range(chunks)] +
                     [(wo_hbm, wo.at[1]), (wg_hbm, wg.at[1]), (wu_hbm, wu.at[1]), (wd_hbm, wd.at[1])]):
        pair.append(remote(src, dst, s_pair_s.at[len(pair)], s_pair_r.at[len(pair)], partner))
        pair[-1].start()

    full, rest = vocab // TILE, vocab % TILE
    count = full + 1
    assert full % 2 == 1 and rest % STEP == 0 and rest > 0

    def tile_copy(p, i, size):
        slot = (p * count + i) % 3
        start = i * TILE if isinstance(i, int) else pl.multiple_of(i * TILE, TILE)
        return pltpu.make_async_copy(lm_hbm.at[pl.ds(start, size)], tiles.at[slot, pl.ds(0, size)], s_tile.at[slot])

    tile_copy(0, 0, TILE).start()
    tile_copy(0, 1, TILE).start()

    def project(p):
        @pl.loop(0, model // COLS)
        def _(n):
            cols = pl.ds(pl.multiple_of(n * COLS, COLS), COLS)
            acc = jnp.dot(att_own[quad(p), :], wo[0, :, cols], preferred_element_type=F32)
            acc = acc + jnp.dot(att_far[quad(p), :], wo[1, :, cols], preferred_element_type=F32)
            part[0, quad(p), cols] = acc.astype(BF16)

    def rs_copies(ph, p):
        mine = part.at[ph]
        half = rows[p] // 2
        sem = lambda k: (s_rs_s.at[ph, p, k], s_rs_r.at[ph, p, k])
        top, low = pl.ds(base[p], half), pl.ds(base[p] + half, half)
        plan = [
            lambda: (mine.at[block(p, x + 2, 0, half)], mrg_in.at[ph, 0, front(p)], *sem(0), right),
            lambda: (mine.at[block(p, x + 2, half, half)], mrg_in.at[ph, 1, front(p)], *sem(1), left),
            lambda: (mine.at[block(p, x + 1, half, half)], fin_in.at[ph, 0, low], *sem(2), right),
            lambda: (mine.at[block(p, x + 3, 0, half)], fin_in.at[ph, 1, top], *sem(3), left),
            lambda: (mrg_out.at[ph, 0, front(p)], fin_in.at[ph, 0, top], *sem(4), right),
            lambda: (mrg_out.at[ph, 1, front(p)], fin_in.at[ph, 1, low], *sem(5), left),
        ]
        return Copies(remote, plan)

    def rs_start(ph, p):
        for k in range(4):
            rs_copies(ph, p)[k].start()

    def rs_merge(ph, p):
        c = rs_copies(ph, p)
        half = rows[p] // 2
        c[0].wait_recv()
        mrg_out[ph, 0, front(p), :] = (part[ph, block(p, x + 1, 0, half), :].astype(F32) + mrg_in[ph, 0, front(p), :].astype(F32)).astype(BF16)
        c[4].start()
        c[1].wait_recv()
        mrg_out[ph, 1, front(p), :] = (part[ph, block(p, x + 3, half, half), :].astype(F32) + mrg_in[ph, 1, front(p), :].astype(F32)).astype(BF16)
        c[5].start()

    def rs_finish(ph, p):
        c = rs_copies(ph, p)
        for k in (2, 3, 4, 5):
            c[k].wait_recv()
        total = part[ph, block(p, x, 0, rows[p]), :].astype(F32) + fin_in[ph, 0, own(p), :].astype(F32) + fin_in[ph, 1, own(p), :].astype(F32)
        return total.astype(BF16).astype(F32)

    def ag_copies(ph, p):
        half = rows[p] // 2
        if ph == 0:
            at = lambda b, lo: gat.at[block(p, b, lo, half)]
        else:
            at = lambda b, lo: fin.at[placed(p, b, lo, half)]
        sem = lambda k: (s_ag_s.at[ph, p, k], s_ag_r.at[ph, p, k])
        plan = [(x, 0, right), (x, half, right), (x, half, left), (x, 0, left), (x + 3, 0, right), (x + 1, half, left)]
        return Copies(remote, [lambda k=k, b=b, lo=lo, dev=dev: (at(b, lo), at(b, lo), *sem(k), dev) for k, (b, lo, dev) in enumerate(plan)])

    def dd_copies(p):
        def plan(k):
            at = fin.at[placed(p, x + k, 0, rows[p])]
            return at, at, s_dd_s.at[p, k], s_dd_r.at[p, k], partner

        return Copies(remote, [functools.partial(plan, k) for k in range(CHIPS)])

    def ag_start(ph, p):
        c = ag_copies(ph, p)
        for k in (0, 2, 1, 3):
            c[k].start()
        if ph == 1:
            dd_copies(p)[0].start()

    def ag_forward(ph, p):
        c = ag_copies(ph, p)
        c[0].wait_recv()
        c[4].start()
        c[2].wait_recv()
        c[5].start()

    def ag_wait(ph, p):
        c = ag_copies(ph, p)
        d = dd_copies(p)
        c[1].wait_recv()
        if ph == 1:
            d[3].start()
        c[3].wait_recv()
        if ph == 1:
            d[1].start()
        c[4].wait_recv()
        c[5].wait_recv()
        if ph == 1:
            d[2].start()

    def dd_wait(p):
        for d in dd_copies(p).all():
            d.wait_recv()

    def attn_end(p):
        summed = rs_finish(0, p)
        res = (hid[own(p), :].astype(F32) + summed).astype(BF16)
        h1[own(p), :] = res
        gat[block(p, x, 0, rows[p]), :] = rms_norm(res, gain_m[...].reshape(1, -1))
        ag_start(0, p)

    def mlp_end(p):
        summed = rs_finish(1, p)
        res = (h1[own(p), :].astype(F32) + summed).astype(BF16)
        fin[placed(p, x, 0, rows[p]), :] = rms_norm(res, gain_f[...].reshape(1, -1))
        ag_start(1, p)

    def mlp(p, between=None):
        ffn = wg.shape[-1]
        used = pl.ds(0, CHIPS * rows[p])
        for s in range(2):
            @pl.loop(0, ffn // COLS)
            def _(n):
                cols = pl.ds(pl.multiple_of(n * COLS, COLS), COLS)
                gate = jnp.dot(gat[quad(p), :], wg[s, :, cols], preferred_element_type=F32)
                upper = jnp.dot(gat[quad(p), :], wu[s, :, cols], preferred_element_type=F32)
                act[s, used, cols] = (jax.nn.silu(gate) * upper).astype(BF16)

            if s == 0 and between is not None:
                between()

        @pl.loop(0, model // COLS)
        def _(n):
            cols = pl.ds(pl.multiple_of(n * COLS, COLS), COLS)
            acc = jnp.dot(act[0, used, :], wd[0, :, cols], preferred_element_type=F32)
            acc = acc + jnp.dot(act[1, used, :], wd[1, :, cols], preferred_element_type=F32)
            part[1, quad(p), cols] = acc.astype(BF16)

    def multiply(p, i, size, out):
        slot = (p * count + i) % 3
        tile_copy(p, i, size).wait()
        span = 2 * CHIPS * rows[p]
        cut = size if span > 256 else size // 2
        for r in range(0, size, cut):
            out[pl.ds(r, cut), pl.ds(0, span)] = lax.dot_general(
                tiles[slot, pl.ds(r, cut), :], fin[wide(p), :], (((1,), (1,)), ((), ())), preferred_element_type=F32)

    def fold(p, i, size, src):
        span = 2 * CHIPS * rows[p]
        cols = pl.ds(0, span)
        goal = target[:, wide(p)] - (me * vocab + i * TILE) - lax.broadcasted_iota(jnp.int32, (8, span), 0)
        depth = STEP // 8
        offsets = 8 * lax.broadcasted_iota(jnp.int32, (depth, 8, span), 0)
        old = run[0, :, cols]
        top = old
        for r in range(0, size, STEP):
            top = jnp.maximum(top, jnp.max(src[pl.ds(r, STEP), cols].reshape(depth, 8, span), axis=0))
        total = run[1, :, cols] * jnp.exp(old - top)
        chosen = run[2, :, cols]
        for r in range(0, size, STEP):
            piece = src[pl.ds(r, STEP), cols].reshape(depth, 8, span)
            total = total + jnp.sum(jnp.exp(piece - top[None]), axis=0)
            chosen = chosen + jnp.sum(jnp.where((goal - r)[None] == offsets, piece, 0.0), axis=0)
        run[0, :, cols] = top
        run[1, :, cols] = total
        run[2, :, cols] = chosen

    def prefetch(p, i):
        @pl.when(i < full)
        def _():
            tile_copy(p, i, TILE).start()

        @pl.when(i == full)
        def _():
            tile_copy(p, full, rest).start()

    def head(p, events):
        run[0] = jnp.full(run.shape[1:], -jnp.inf, F32)
        run[1] = jnp.zeros(run.shape[1:], F32)
        run[2] = jnp.zeros(run.shape[1:], F32)
        tile_copy(p, 2, TILE).start()
        multiply(p, 0, TILE, lga)

        @pl.loop(0, full // 2)
        def _(j):
            for when, event in events:
                pl.when(j == when)(event)
            i = 2 * j
            prefetch(p, i + 3)
            multiply(p, i + 1, TILE, lgb)
            fold(p, i, TILE, lga)
            prefetch(p, i + 4)
            multiply(p, i + 2, TILE, lga)
            fold(p, i + 1, TILE, lgb)

        if p + 1 < chunks:
            tile_copy(p + 1, 0, TILE).start()
            tile_copy(p + 1, 1, TILE).start()
        multiply(p, full, rest, lgb)
        fold(p, full - 1, TILE, lga)
        fold(p, full, rest, lgb)
        span = 2 * CHIPS * rows[p]
        cols = pl.ds(0, span)
        top = jnp.max(run[0, :, cols], axis=0, keepdims=True)
        total = jnp.sum(run[1, :, cols] * jnp.exp(run[0, :, cols] - top), axis=0, keepdims=True)
        chosen = jnp.sum(run[2, :, cols], axis=0, keepdims=True)
        for k, row in enumerate((top, total, chosen)):
            for g in range(span // 128):
                stats[me, k, pl.ds(2 * CHIPS * base[p] // 128 + g, 1), :] = row[:, g * 128:(g + 1) * 128]

    def wait_loads(lo, hi):
        for k in range(lo, hi):
            loads[k].wait()

    wait_loads(0, chunks + 1)
    for k in range(chunks):
        pair[k].wait_recv()
    pair[chunks].wait_recv()
    project(0)
    rs_start(0, 0)
    wait_loads(chunks + 1, 2 * chunks + 1)
    project(1)
    project(2)
    rs_merge(0, 0)
    attn_end(0)
    ag_forward(0, 0)
    rs_start(0, 1)
    wait_loads(2 * chunks + 1, len(loads))
    for k in (1, 2, 3):
        pair[chunks + k].wait_recv()
    ag_wait(0, 0)
    mlp(0, lambda: rs_merge(0, 1))
    rs_start(1, 0)
    rs_merge(1, 0)
    mlp_end(0)
    ag_forward(1, 0)
    attn_end(1)
    ag_wait(1, 0)
    dd_wait(0)

    def forward_and_start():
        ag_forward(0, 1)
        rs_start(0, 2)

    def feed(p):
        ag_wait(0, p)
        mlp(p)
        rs_start(1, p)

    def forward_and_end():
        ag_forward(1, 1)
        attn_end(2)

    head(0, [(0, forward_and_start), (1, lambda: feed(1)), (2, lambda: rs_merge(0, 2)), (3, lambda: rs_merge(1, 1)),
             (4, lambda: mlp_end(1)), (5, forward_and_end), (6, lambda: ag_wait(1, 1))])
    dd_wait(1)
    head(1, [(0, lambda: ag_forward(0, 2)), (1, lambda: feed(2)), (3, lambda: rs_merge(1, 2)), (4, lambda: mlp_end(2)),
             (6, lambda: ag_forward(1, 2))])
    ag_wait(1, 2)
    dd_wait(2)
    head(2, [])

    sent = []
    for k in range(1, tp):
        sent.append(remote(stats.at[me], stats.at[me], s_st_s.at[k - 1], s_st_r.at[k - 1], (me + k) % tp))
        sent[-1].start()
    for d in sent:
        d.wait_recv()
    top = stats[0, 0]
    for k in range(1, tp):
        top = jnp.maximum(top, stats[k, 0])
    total = jnp.zeros_like(top)
    chosen = jnp.zeros_like(top)
    for k in range(tp):
        total = total + stats[k, 1] * jnp.exp(stats[k, 0] - top)
        chosen = chosen + stats[k, 2]
    log_norm = top + jnp.log(total)
    norm_out[...] = log_norm
    prob_out[...] = chosen - log_norm

    for d in sent + pair:
        d.wait_send()
    for p in range(chunks):
        for ph in range(2):
            for d in rs_copies(ph, p).all() + ag_copies(ph, p).all():
                d.wait_send()
        for d in dd_copies(p).all():
            d.wait_send()


def tail(tp, attended, hidden, w_o, w_gate, w_up, w_down, w_lm, mlp_norm, final_norm, score_id):
    tokens, model = hidden.shape
    heads = attended.shape[-1]
    ffn = w_gate.shape[-1]
    chunks = len(SHARES)
    rows = tokens // tp
    quad = CHIPS * rows
    most = tokens * max(SHARES) // sum(SHARES)
    target = jnp.broadcast_to(score_id.reshape(1, tokens), (8, tokens))
    anyspace = pl.BlockSpec(memory_space=pl.ANY)
    vmem = pl.BlockSpec(memory_space=pltpu.VMEM)
    dma = pltpu.SemaphoreType.DMA
    flops = 2 * tokens * model * (w_lm.shape[-1] + 3 * ffn + heads)
    log_norm, log_prob = pl.pallas_call(
        functools.partial(tail_body, tp),
        out_shape=[jax.ShapeDtypeStruct((tokens // 128, 128), F32)] * 2,
        in_specs=[anyspace] * 7 + [vmem] * 3,
        out_specs=[vmem] * 2,
        scratch_shapes=[
            pltpu.VMEM((quad, heads), BF16), pltpu.VMEM((quad, heads), BF16),
            pltpu.VMEM((rows, model), BF16), pltpu.VMEM((2, heads, model), BF16),
            pltpu.VMEM((2, model, ffn), BF16), pltpu.VMEM((2, model, ffn), BF16), pltpu.VMEM((2, ffn, model), BF16),
            pltpu.VMEM((2, quad, model), BF16), pltpu.VMEM((2, 2, rows // 2, model), BF16),
            pltpu.VMEM((2, 2, rows // 2, model), BF16), pltpu.VMEM((2, 2, rows, model), BF16),
            pltpu.VMEM((rows, model), BF16), pltpu.VMEM((quad, model), BF16),
            pltpu.VMEM((tokens, model), BF16), pltpu.VMEM((2, most // 2, ffn), BF16),
            pltpu.VMEM((3, TILE, model), BF16), pltpu.VMEM((TILE, most), F32), pltpu.VMEM((TILE, most), F32),
            pltpu.VMEM((3, 8, most), F32), pltpu.VMEM((tp, 3, tokens // 128, 128), F32),
            dma((2 * chunks + 4,)), dma((chunks + 4,)), dma((chunks + 4,)),
            dma((2, chunks, 6)), dma((2, chunks, 6)), dma((2, chunks, 6)), dma((2, chunks, 6)),
            dma((chunks, CHIPS)), dma((chunks, CHIPS)), dma((3,)), dma((tp - 1,)), dma((tp - 1,)),
        ],
        compiler_params=pltpu.CompilerParams(collective_id=0, has_side_effects=True, vmem_limit_bytes=VMEM_LIMIT),
        cost_estimate=pl.CostEstimate(flops=flops, bytes_accessed=2 * chunks * w_lm.size, transcendentals=tokens * w_lm.shape[-1]),
        name="layer_tail_and_head",
    )(attended, hidden, w_o, w_gate, w_up, w_down, w_lm.T, mlp_norm, final_norm, target)
    return log_norm, log_prob


def solution(mesh):
    tp = mesh.shape["tp"]

    def group_step(hidden, tree_mask, depth, ctx_len, block_table, score_id, k_cache, v_cache, attn_norm, w_q, w_k, w_v, w_o, mlp_norm, w_gate, w_up, w_down, final_norm, w_lm):
        requests, nodes, model = hidden.shape
        attended, k_out, v_out = attention(hidden, tree_mask, depth, ctx_len, block_table, k_cache, v_cache, attn_norm, w_q, w_k, w_v)
        log_norm, log_prob = tail(tp, attended, hidden.reshape(requests * nodes, model), w_o, w_gate, w_up, w_down, w_lm, mlp_norm, final_norm, score_id)
        return log_norm.reshape(requests, nodes), log_prob.reshape(requests, nodes), k_out, v_out

    request_spec = P("dp", None, None)
    node_spec = P("dp", None)
    cache_spec = P("dp", None, "tp", None)
    shared_spec = P(None)
    column_spec = P(None, "tp")
    row_spec = P("tp", None)
    in_specs = (request_spec, request_spec, node_spec, P("dp"), node_spec, node_spec, cache_spec, cache_spec, shared_spec, column_spec, column_spec, column_spec, row_spec, shared_spec, column_spec, column_spec, row_spec, shared_spec, column_spec)
    out_specs = (node_spec, node_spec, cache_spec, cache_spec)
    return jax.shard_map(group_step, mesh=mesh, in_specs=in_specs, out_specs=out_specs, check_vma=False)
```

```python
import functools

import jax
import jax.numpy as jnp
from jax import lax
from jax.experimental import pallas as pl
from jax.experimental.pallas import tpu as pltpu
from jax.sharding import PartitionSpec as P

RMS_EPS = 1e-5
ROPE_THETA = 500000
CHIPS = 4
PER_STEP = 4
SHARES = (1, 1, 2)
TILE = 1024
COLS = 512
STEP = 32
VMEM_LIMIT = 67043328
F32 = jnp.float32
BF16 = jnp.bfloat16


def rms_norm(values, gain):
    widened = values.astype(F32)
    scale = lax.rsqrt(jnp.mean(widened * widened, axis=-1, keepdims=True) + RMS_EPS)
    return (widened * scale * gain.astype(F32)).astype(BF16)


def attention_body(per, pages, ctx, table, hidden, gain, w_q, w_k, w_v, cosine, sine, mask, k_in, v_in, att, k_out, v_out, w_kv, q_heads, kv_old, kv):
    step = pl.program_id(0)
    nodes = mask.shape[1]
    size, dim, blocks = k_in.shape
    lanes = 2 * dim
    pitch = kv.shape[0] // size
    heads = w_q.shape[1] // dim
    span = pages * size

    @pl.when(step == 0)
    def _():
        w_kv[pl.ds(0, dim), :] = w_k[...]
        w_kv[pl.ds(dim, dim), :] = w_v[...]
        for s in range(size):
            joined = jnp.concatenate([k_in[s].astype(F32), v_in[s].astype(F32)], axis=0)
            kv[pl.ds(s * pitch, blocks), :] = joined.T

    normed = rms_norm(hidden[...], gain[...].reshape(1, -1))
    nt = (((1,), (1,)), ((), ()))
    queries = jnp.dot(normed, w_q[...], preferred_element_type=F32)
    pair = lax.dot_general(normed, w_kv[...], nt, preferred_element_type=F32)
    lane = lax.broadcasted_iota(jnp.int32, (per * nodes, lanes), 1)
    lower = (lane % dim) < dim // 2

    def rotate(values):
        swapped = jnp.where(lower, pltpu.roll(values, lanes - dim // 2, 1), pltpu.roll(values, dim // 2, 1))
        return values * cosine[...] + swapped * sine[...]

    for h in range(0, heads, 2):
        turned = rotate(queries[:, h * dim:(h + 2) * dim])
        q_heads[h] = jnp.where(lane < dim, turned, 0.0).astype(BF16)
        q_heads[h + 1] = jnp.where(lane < dim, pltpu.roll(turned, dim, 1), 0.0).astype(BF16)
    pair = jnp.where(lane < dim, rotate(pair), pair).astype(BF16)
    scale = dim ** -0.5
    slot = lax.broadcasted_iota(jnp.int32, (heads * nodes, span), 1)
    row = lax.broadcasted_iota(jnp.int32, (size, lanes), 0)
    for r in range(per):
        b = step * per + r
        length = ctx[b]
        for j in range(pages):
            kv_old[r, pl.ds(j * size, size), :] = kv[pl.ds(table[b, j], size, stride=pitch), :].astype(BF16)
        fresh = pair[r * nodes:(r + 1) * nodes]
        query = q_heads[:, pl.ds(r * nodes, nodes), :].reshape(heads * nodes, lanes)
        score_old = lax.dot_general(query, kv_old[r], nt, preferred_element_type=F32) * scale
        score_old = jnp.where(slot < length, score_old, -jnp.inf)
        score_new = lax.dot_general(query, fresh, nt, preferred_element_type=F32) * scale
        seen = jnp.broadcast_to((mask[r] > 0)[None], (heads, nodes, nodes)).reshape(heads * nodes, nodes)
        score_new = jnp.where(seen, score_new, -jnp.inf)
        top = jnp.maximum(jnp.max(score_old, axis=-1, keepdims=True), jnp.max(score_new, axis=-1, keepdims=True))
        prob_old = jnp.exp(score_old - top)
        prob_new = jnp.exp(score_new - top)
        total = jnp.sum(prob_old, axis=-1, keepdims=True) + jnp.sum(prob_new, axis=-1, keepdims=True)
        mixed = jnp.dot(prob_old.astype(BF16), kv_old[r], preferred_element_type=F32)
        mixed = mixed + jnp.dot(prob_new.astype(BF16), fresh, preferred_element_type=F32)
        mixed = mixed / total
        for h in range(0, heads, 2):
            even = pltpu.roll(mixed[h * nodes:(h + 1) * nodes], dim, 1)
            odd = mixed[(h + 1) * nodes:(h + 2) * nodes]
            joined = jnp.where(lane[:nodes] < dim, even, odd)
            att[pl.ds(r * nodes, nodes), h * dim:(h + 2) * dim] = joined.astype(BF16)

        shift = length % size
        window = jnp.concatenate([fresh.astype(F32), jnp.zeros((size, lanes), F32)], axis=0)
        window = pltpu.roll(window, shift, 0)
        for j in range(nodes // size + 1):
            page = table[b, jnp.minimum(length // size + j, pages - 1)]
            place = row + j * size
            fits = (place >= shift) & (place < shift + nodes)
            at = pl.ds(page, size, stride=pitch)
            kv[at, :] = jnp.where(fits, window[j * size:(j + 1) * size], kv[at, :])

    @pl.when(step == pl.num_programs(0) - 1)
    def _():
        for s in range(size):
            apart = kv[pl.ds(s * pitch, blocks), :].T.astype(BF16)
            k_out[s] = apart[:dim]
            v_out[s] = apart[dim:]


def attention(hidden, tree_mask, depth, ctx_len, block_table, k_cache, v_cache, attn_norm, w_q, w_k, w_v):
    requests, nodes, model = hidden.shape
    blocks, size, kv_local, dim = k_cache.shape
    pages = block_table.shape[1]
    per = PER_STEP
    rows = per * nodes
    heads = w_q.shape[1] // dim
    half = dim // 2
    lane = jnp.arange(2 * dim)
    inv_freq = 1.0 / (ROPE_THETA ** ((lane % half).astype(F32) * (2.0 / dim)))
    angles = (ctx_len[:, None] + depth).astype(F32)[..., None] * inv_freq
    cosine = jnp.cos(angles).reshape(requests * nodes, 2 * dim)
    sine = (jnp.sin(angles) * jnp.where(lane % dim < half, -1.0, 1.0)).reshape(requests * nodes, 2 * dim)
    stored = lambda cache: cache.transpose(1, 2, 3, 0).reshape(size, dim, blocks)
    native = lambda cache: cache.reshape(size, kv_local, dim, blocks).transpose(3, 0, 1, 2)
    cache_type = jax.ShapeDtypeStruct((size, dim, blocks), BF16)
    whole = lambda *shape: pl.BlockSpec(shape, lambda i, *_: (0,) * len(shape))
    by_row = lambda width: pl.BlockSpec((rows, width), lambda i, *_: (i, 0))
    att, k_out, v_out = pl.pallas_call(
        functools.partial(attention_body, per, pages),
        out_shape=[jax.ShapeDtypeStruct((requests * nodes, heads * dim), BF16), cache_type, cache_type],
        grid_spec=pltpu.PrefetchScalarGridSpec(
            num_scalar_prefetch=2,
            grid=(requests // per,),
            in_specs=[by_row(model), whole(model), whole(model, heads * dim), whole(dim, model), whole(dim, model),
                      by_row(2 * dim), by_row(2 * dim), pl.BlockSpec((per, nodes, nodes), lambda i, *_: (i, 0, 0)),
                      whole(size, dim, blocks), whole(size, dim, blocks)],
            out_specs=[by_row(heads * dim), whole(size, dim, blocks), whole(size, dim, blocks)],
            scratch_shapes=[pltpu.VMEM((2 * dim, model), BF16), pltpu.VMEM((heads, rows, 2 * dim), BF16),
                            pltpu.VMEM((per, pages * size, 2 * dim), BF16), pltpu.VMEM((size * (blocks + 8), 2 * dim), F32)],
        ),
        compiler_params=pltpu.CompilerParams(vmem_limit_bytes=VMEM_LIMIT),
        cost_estimate=pl.CostEstimate(flops=2 * requests * nodes * model * (heads + 2) * dim, bytes_accessed=hidden.size * 2, transcendentals=0),
        name="tree_attention",
    )(ctx_len, block_table, hidden.reshape(requests * nodes, model), attn_norm, w_q, w_k.T, w_v.T,
      cosine, sine, tree_mask, stored(k_cache), stored(v_cache))
    return att, native(k_out), native(v_out)


class Copies:
    def __init__(self, make, plan):
        self.make = make
        self.plan = plan

    def __getitem__(self, k):
        return self.make(*self.plan[k]())

    def all(self):
        return [self[k] for k in range(len(self.plan))]


def tail_body(tp, att_hbm, hid_hbm, wo_hbm, wg_hbm, wu_hbm, wd_hbm, lm_hbm, gain_m, gain_f, target, norm_out, prob_out,
              att_own, att_far, hid, wo, wg, wu, wd, part, mrg_in, mrg_out, fin_in, h1, gat, fin, act, tiles, lga, lgb, run, stats,
              s_load, s_pair_s, s_pair_r, s_rs_s, s_rs_r, s_ag_s, s_ag_r, s_dd_s, s_dd_r, s_tile, s_st_s, s_st_r):
    me = lax.axis_index("tp")
    x = me // 2
    core = me % 2
    right = 2 * ((x + 1) % CHIPS) + core
    left = 2 * ((x + CHIPS - 1) % CHIPS) + core
    partner = me + 1 - 2 * core
    chunks = len(SHARES)
    rows = [h1.shape[0] * share // sum(SHARES) for share in SHARES]
    base = [sum(rows[:p]) for p in range(chunks)]
    vocab = lm_hbm.shape[0]
    model = hid.shape[-1]

    def own(p):
        return pl.ds(base[p], rows[p])

    def quad(p):
        return pl.ds(CHIPS * base[p], CHIPS * rows[p])

    def wide(p):
        return pl.ds(2 * CHIPS * base[p], 2 * CHIPS * rows[p])

    def front(p):
        return pl.ds(base[p] // 2, rows[p] // 2)

    def block(p, b, lo, n):
        return pl.ds(pl.multiple_of(CHIPS * base[p] + (b % CHIPS) * rows[p] + lo, rows[p] // 2), n)

    def placed(p, b, lo, n):
        return pl.ds(pl.multiple_of(CHIPS * (2 * base[p] + core * rows[p]) + (b % CHIPS) * rows[p] + lo, rows[p] // 2), n)

    def remote(src, dst, ssem, rsem, dev):
        return pltpu.make_async_remote_copy(src_ref=src, dst_ref=dst, send_sem=ssem, recv_sem=rsem,
                                            device_id={"tp": dev}, device_id_type=pl.DeviceIdType.MESH)

    barrier = pltpu.get_barrier_semaphore()
    for k in range(1, tp):
        pl.semaphore_signal(barrier, inc=1, device_id={"tp": (me + k) % tp}, device_id_type=pl.DeviceIdType.MESH)

    def token_rows(p, c):
        return pl.ds(pl.multiple_of(CHIPS * (2 * base[p] + c * rows[p]), CHIPS * rows[p]), CHIPS * rows[p])

    loads = []

    def load(src, dst):
        loads.append(pltpu.make_async_copy(src, dst, s_load.at[len(loads)]))
        loads[-1].start()

    for p in range(chunks):
        load(att_hbm.at[token_rows(p, core)], att_own.at[quad(p)])
    load(wo_hbm, wo.at[0])
    for p in range(chunks):
        load(hid_hbm.at[placed(p, x, 0, rows[p])], hid.at[own(p)])
    load(wg_hbm, wg.at[0])
    load(wu_hbm, wu.at[0])
    load(wd_hbm, wd.at[0])

    pl.semaphore_wait(barrier, tp - 1)

    pair = []
    for src, dst in ([(att_hbm.at[token_rows(p, 1 - core)], att_far.at[quad(p)]) for p in range(chunks)] +
                     [(wo_hbm, wo.at[1]), (wg_hbm, wg.at[1]), (wu_hbm, wu.at[1]), (wd_hbm, wd.at[1])]):
        pair.append(remote(src, dst, s_pair_s.at[len(pair)], s_pair_r.at[len(pair)], partner))
        pair[-1].start()

    full, rest = vocab // TILE, vocab % TILE
    count = full + 1
    assert full % 2 == 1 and rest % STEP == 0 and rest > 0

    def tile_copy(p, i, size):
        slot = (p * count + i) % 3
        start = i * TILE if isinstance(i, int) else pl.multiple_of(i * TILE, TILE)
        return pltpu.make_async_copy(lm_hbm.at[pl.ds(start, size)], tiles.at[slot, pl.ds(0, size)], s_tile.at[slot])

    tile_copy(0, 0, TILE).start()
    tile_copy(0, 1, TILE).start()

    def project(p):
        @pl.loop(0, model // COLS)
        def _(n):
            cols = pl.ds(pl.multiple_of(n * COLS, COLS), COLS)
            acc = jnp.dot(att_own[quad(p), :], wo[0, :, cols], preferred_element_type=F32)
            acc = acc + jnp.dot(att_far[quad(p), :], wo[1, :, cols], preferred_element_type=F32)
            part[0, quad(p), cols] = acc.astype(BF16)

    def rs_copies(ph, p):
        mine = part.at[ph]
        half = rows[p] // 2
        sem = lambda k: (s_rs_s.at[ph, p, k], s_rs_r.at[ph, p, k])
        top, low = pl.ds(base[p], half), pl.ds(base[p] + half, half)
        plan = [
            lambda: (mine.at[block(p, x + 2, 0, half)], mrg_in.at[ph, 0, front(p)], *sem(0), right),
            lambda: (mine.at[block(p, x + 2, half, half)], mrg_in.at[ph, 1, front(p)], *sem(1), left),
            lambda: (mine.at[block(p, x + 1, half, half)], fin_in.at[ph, 0, low], *sem(2), right),
            lambda: (mine.at[block(p, x + 3, 0, half)], fin_in.at[ph, 1, top], *sem(3), left),
            lambda: (mrg_out.at[ph, 0, front(p)], fin_in.at[ph, 0, top], *sem(4), right),
            lambda: (mrg_out.at[ph, 1, front(p)], fin_in.at[ph, 1, low], *sem(5), left),
        ]
        return Copies(remote, plan)

    def rs_start(ph, p):
        for k in range(4):
            rs_copies(ph, p)[k].start()

    def rs_merge(ph, p):
        c = rs_copies(ph, p)
        half = rows[p] // 2
        c[0].wait_recv()
        mrg_out[ph, 0, front(p), :] = (part[ph, block(p, x + 1, 0, half), :].astype(F32) + mrg_in[ph, 0, front(p), :].astype(F32)).astype(BF16)
        c[4].start()
        c[1].wait_recv()
        mrg_out[ph, 1, front(p), :] = (part[ph, block(p, x + 3, half, half), :].astype(F32) + mrg_in[ph, 1, front(p), :].astype(F32)).astype(BF16)
        c[5].start()

    def rs_finish(ph, p):
        c = rs_copies(ph, p)
        for k in (2, 3, 4, 5):
            c[k].wait_recv()
        total = part[ph, block(p, x, 0, rows[p]), :].astype(F32) + fin_in[ph, 0, own(p), :].astype(F32) + fin_in[ph, 1, own(p), :].astype(F32)
        return total.astype(BF16).astype(F32)

    def ag_copies(ph, p):
        half = rows[p] // 2
        if ph == 0:
            at = lambda b, lo: gat.at[block(p, b, lo, half)]
        else:
            at = lambda b, lo: fin.at[placed(p, b, lo, half)]
        sem = lambda k: (s_ag_s.at[ph, p, k], s_ag_r.at[ph, p, k])
        plan = [(x, 0, right), (x, half, right), (x, half, left), (x, 0, left), (x + 3, 0, right), (x + 1, half, left)]
        return Copies(remote, [lambda k=k, b=b, lo=lo, dev=dev: (at(b, lo), at(b, lo), *sem(k), dev) for k, (b, lo, dev) in enumerate(plan)])

    def dd_copies(p):
        def plan(k):
            at = fin.at[placed(p, x + k, 0, rows[p])]
            return at, at, s_dd_s.at[p, k], s_dd_r.at[p, k], partner

        return Copies(remote, [functools.partial(plan, k) for k in range(CHIPS)])

    def ag_start(ph, p):
        c = ag_copies(ph, p)
        for k in (0, 2, 1, 3):
            c[k].start()
        if ph == 1:
            dd_copies(p)[0].start()

    def ag_forward(ph, p):
        c = ag_copies(ph, p)
        c[0].wait_recv()
        c[4].start()
        c[2].wait_recv()
        c[5].start()

    def ag_wait(ph, p):
        c = ag_copies(ph, p)
        d = dd_copies(p)
        c[1].wait_recv()
        if ph == 1:
            d[3].start()
        c[3].wait_recv()
        if ph == 1:
            d[1].start()
        c[4].wait_recv()
        c[5].wait_recv()
        if ph == 1:
            d[2].start()

    def dd_wait(p):
        for d in dd_copies(p).all():
            d.wait_recv()

    def attn_end(p):
        summed = rs_finish(0, p)
        res = (hid[own(p), :].astype(F32) + summed).astype(BF16)
        h1[own(p), :] = res
        gat[block(p, x, 0, rows[p]), :] = rms_norm(res, gain_m[...].reshape(1, -1))
        ag_start(0, p)

    def mlp_end(p):
        summed = rs_finish(1, p)
        res = (h1[own(p), :].astype(F32) + summed).astype(BF16)
        fin[placed(p, x, 0, rows[p]), :] = rms_norm(res, gain_f[...].reshape(1, -1))
        ag_start(1, p)

    def mlp(p, between=None):
        ffn = wg.shape[-1]
        used = pl.ds(0, CHIPS * rows[p])
        for s in range(2):
            @pl.loop(0, ffn // COLS)
            def _(n):
                cols = pl.ds(pl.multiple_of(n * COLS, COLS), COLS)
                gate = jnp.dot(gat[quad(p), :], wg[s, :, cols], preferred_element_type=F32)
                upper = jnp.dot(gat[quad(p), :], wu[s, :, cols], preferred_element_type=F32)
                act[s, used, cols] = (jax.nn.silu(gate) * upper).astype(BF16)

            if s == 0 and between is not None:
                between()

        @pl.loop(0, model // COLS)
        def _(n):
            cols = pl.ds(pl.multiple_of(n * COLS, COLS), COLS)
            acc = jnp.dot(act[0, used, :], wd[0, :, cols], preferred_element_type=F32)
            acc = acc + jnp.dot(act[1, used, :], wd[1, :, cols], preferred_element_type=F32)
            part[1, quad(p), cols] = acc.astype(BF16)

    def multiply(p, i, size, out):
        slot = (p * count + i) % 3
        tile_copy(p, i, size).wait()
        span = 2 * CHIPS * rows[p]
        cut = size if span > 256 else size // 2
        for r in range(0, size, cut):
            out[pl.ds(r, cut), pl.ds(0, span)] = lax.dot_general(
                tiles[slot, pl.ds(r, cut), :], fin[wide(p), :], (((1,), (1,)), ((), ())), preferred_element_type=F32)

    def fold(p, i, size, src):
        span = 2 * CHIPS * rows[p]
        cols = pl.ds(0, span)
        goal = target[:, wide(p)] - (me * vocab + i * TILE) - lax.broadcasted_iota(jnp.int32, (8, span), 0)
        depth = STEP // 8
        offsets = 8 * lax.broadcasted_iota(jnp.int32, (depth, 8, span), 0)
        old = run[0, :, cols]
        top = old
        for r in range(0, size, STEP):
            top = jnp.maximum(top, jnp.max(src[pl.ds(r, STEP), cols].reshape(depth, 8, span), axis=0))
        total = run[1, :, cols] * jnp.exp(old - top)
        chosen = run[2, :, cols]
        for r in range(0, size, STEP):
            piece = src[pl.ds(r, STEP), cols].reshape(depth, 8, span)
            total = total + jnp.sum(jnp.exp(piece - top[None]), axis=0)
            chosen = chosen + jnp.sum(jnp.where((goal - r)[None] == offsets, piece, 0.0), axis=0)
        run[0, :, cols] = top
        run[1, :, cols] = total
        run[2, :, cols] = chosen

    def prefetch(p, i):
        @pl.when(i < full)
        def _():
            tile_copy(p, i, TILE).start()

        @pl.when(i == full)
        def _():
            tile_copy(p, full, rest).start()

    def head(p, events):
        run[0] = jnp.full(run.shape[1:], -jnp.inf, F32)
        run[1] = jnp.zeros(run.shape[1:], F32)
        run[2] = jnp.zeros(run.shape[1:], F32)
        tile_copy(p, 2, TILE).start()
        multiply(p, 0, TILE, lga)

        @pl.loop(0, full // 2)
        def _(j):
            for when, event in events:
                pl.when(j == when)(event)
            i = 2 * j
            prefetch(p, i + 3)
            multiply(p, i + 1, TILE, lgb)
            fold(p, i, TILE, lga)
            prefetch(p, i + 4)
            multiply(p, i + 2, TILE, lga)
            fold(p, i + 1, TILE, lgb)

        if p + 1 < chunks:
            tile_copy(p + 1, 0, TILE).start()
            tile_copy(p + 1, 1, TILE).start()
        multiply(p, full, rest, lgb)
        fold(p, full - 1, TILE, lga)
        fold(p, full, rest, lgb)
        span = 2 * CHIPS * rows[p]
        cols = pl.ds(0, span)
        top = jnp.max(run[0, :, cols], axis=0, keepdims=True)
        total = jnp.sum(run[1, :, cols] * jnp.exp(run[0, :, cols] - top), axis=0, keepdims=True)
        chosen = jnp.sum(run[2, :, cols], axis=0, keepdims=True)
        for k, row in enumerate((top, total, chosen)):
            for g in range(span // 128):
                stats[me, k, pl.ds(2 * CHIPS * base[p] // 128 + g, 1), :] = row[:, g * 128:(g + 1) * 128]

    def wait_loads(lo, hi):
        for k in range(lo, hi):
            loads[k].wait()

    wait_loads(0, chunks + 1)
    for k in range(chunks):
        pair[k].wait_recv()
    pair[chunks].wait_recv()
    project(0)
    rs_start(0, 0)
    wait_loads(chunks + 1, 2 * chunks + 1)
    project(1)
    project(2)
    rs_merge(0, 0)
    attn_end(0)
    ag_forward(0, 0)
    rs_start(0, 1)
    wait_loads(2 * chunks + 1, len(loads))
    ag_wait(0, 0)

    def far_weights():
        rs_merge(0, 1)
        for k in (1, 2, 3):
            pair[chunks + k].wait_recv()

    mlp(0, far_weights)
    rs_start(1, 0)
    rs_merge(1, 0)
    mlp_end(0)
    ag_forward(1, 0)
    attn_end(1)
    ag_wait(1, 0)
    dd_wait(0)

    def forward_and_start():
        ag_forward(0, 1)
        rs_start(0, 2)

    def feed(p):
        ag_wait(0, p)
        mlp(p)
        rs_start(1, p)

    def two_ends():
        mlp_end(1)
        attn_end(2)

    head(0, [(0, forward_and_start), (1, lambda: feed(1)), (2, lambda: rs_merge(0, 2)), (3, lambda: rs_merge(1, 1)),
             (4, two_ends), (6, lambda: ag_forward(1, 1))])
    ag_wait(1, 1)
    dd_wait(1)
    head(1, [(0, lambda: ag_forward(0, 2)), (1, lambda: feed(2)), (3, lambda: rs_merge(1, 2)), (4, lambda: mlp_end(2)),
             (6, lambda: ag_forward(1, 2))])
    ag_wait(1, 2)
    dd_wait(2)
    head(2, [])

    sent = []
    for k in range(1, tp):
        sent.append(remote(stats.at[me], stats.at[me], s_st_s.at[k - 1], s_st_r.at[k - 1], (me + k) % tp))
        sent[-1].start()
    for d in sent:
        d.wait_recv()
    top = stats[0, 0]
    for k in range(1, tp):
        top = jnp.maximum(top, stats[k, 0])
    total = jnp.zeros_like(top)
    chosen = jnp.zeros_like(top)
    for k in range(tp):
        total = total + stats[k, 1] * jnp.exp(stats[k, 0] - top)
        chosen = chosen + stats[k, 2]
    log_norm = top + jnp.log(total)
    norm_out[...] = log_norm
    prob_out[...] = chosen - log_norm

    for d in sent + pair:
        d.wait_send()
    for p in range(chunks):
        for ph in range(2):
            for d in rs_copies(ph, p).all() + ag_copies(ph, p).all():
                d.wait_send()
        for d in dd_copies(p).all():
            d.wait_send()


def tail(tp, attended, hidden, w_o, w_gate, w_up, w_down, w_lm, mlp_norm, final_norm, score_id):
    tokens, model = hidden.shape
    heads = attended.shape[-1]
    ffn = w_gate.shape[-1]
    chunks = len(SHARES)
    rows = tokens // tp
    quad = CHIPS * rows
    most = tokens * max(SHARES) // sum(SHARES)
    target = jnp.broadcast_to(score_id.reshape(1, tokens), (8, tokens))
    anyspace = pl.BlockSpec(memory_space=pl.ANY)
    vmem = pl.BlockSpec(memory_space=pltpu.VMEM)
    dma = pltpu.SemaphoreType.DMA
    flops = 2 * tokens * model * (w_lm.shape[-1] + 3 * ffn + heads)
    log_norm, log_prob = pl.pallas_call(
        functools.partial(tail_body, tp),
        out_shape=[jax.ShapeDtypeStruct((tokens // 128, 128), F32)] * 2,
        in_specs=[anyspace] * 7 + [vmem] * 3,
        out_specs=[vmem] * 2,
        scratch_shapes=[
            pltpu.VMEM((quad, heads), BF16), pltpu.VMEM((quad, heads), BF16),
            pltpu.VMEM((rows, model), BF16), pltpu.VMEM((2, heads, model), BF16),
            pltpu.VMEM((2, model, ffn), BF16), pltpu.VMEM((2, model, ffn), BF16), pltpu.VMEM((2, ffn, model), BF16),
            pltpu.VMEM((2, quad, model), BF16), pltpu.VMEM((2, 2, rows // 2, model), BF16),
            pltpu.VMEM((2, 2, rows // 2, model), BF16), pltpu.VMEM((2, 2, rows, model), BF16),
            pltpu.VMEM((rows, model), BF16), pltpu.VMEM((quad, model), BF16),
            pltpu.VMEM((tokens, model), BF16), pltpu.VMEM((2, most // 2, ffn), BF16),
            pltpu.VMEM((3, TILE, model), BF16), pltpu.VMEM((TILE, most), F32), pltpu.VMEM((TILE, most), F32),
            pltpu.VMEM((3, 8, most), F32), pltpu.VMEM((tp, 3, tokens // 128, 128), F32),
            dma((2 * chunks + 4,)), dma((chunks + 4,)), dma((chunks + 4,)),
            dma((2, chunks, 6)), dma((2, chunks, 6)), dma((2, chunks, 6)), dma((2, chunks, 6)),
            dma((chunks, CHIPS)), dma((chunks, CHIPS)), dma((3,)), dma((tp - 1,)), dma((tp - 1,)),
        ],
        compiler_params=pltpu.CompilerParams(collective_id=0, has_side_effects=True, vmem_limit_bytes=VMEM_LIMIT),
        cost_estimate=pl.CostEstimate(flops=flops, bytes_accessed=2 * chunks * w_lm.size, transcendentals=tokens * w_lm.shape[-1]),
        name="layer_tail_and_head",
    )(attended, hidden, w_o, w_gate, w_up, w_down, w_lm.T, mlp_norm, final_norm, target)
    return log_norm, log_prob


def solution(mesh):
    tp = mesh.shape["tp"]

    def group_step(hidden, tree_mask, depth, ctx_len, block_table, score_id, k_cache, v_cache, attn_norm, w_q, w_k, w_v, w_o, mlp_norm, w_gate, w_up, w_down, final_norm, w_lm):
        requests, nodes, model = hidden.shape
        attended, k_out, v_out = attention(hidden, tree_mask, depth, ctx_len, block_table, k_cache, v_cache, attn_norm, w_q, w_k, w_v)
        log_norm, log_prob = tail(tp, attended, hidden.reshape(requests * nodes, model), w_o, w_gate, w_up, w_down, w_lm, mlp_norm, final_norm, score_id)
        return log_norm.reshape(requests, nodes), log_prob.reshape(requests, nodes), k_out, v_out

    request_spec = P("dp", None, None)
    node_spec = P("dp", None)
    cache_spec = P("dp", None, "tp", None)
    shared_spec = P(None)
    column_spec = P(None, "tp")
    row_spec = P("tp", None)
    in_specs = (request_spec, request_spec, node_spec, P("dp"), node_spec, node_spec, cache_spec, cache_spec, shared_spec, column_spec, column_spec, column_spec, row_spec, shared_spec, column_spec, column_spec, row_spec, shared_spec, column_spec)
    out_specs = (node_spec, node_spec, cache_spec, cache_spec)
    return jax.shard_map(group_step, mesh=mesh, in_specs=in_specs, out_specs=out_specs, check_vma=False)
```
